32 devices in a mesh: solver: 4 (over y, x), space: 8 (over z, core).
Axes of the slice: x: 2, y: 2, z: 4, core: 2. Of those that a mesh axis runs over, the one named last changes fastest.
Arguments:
- pressure_start: float32 [128, 256, 512], P(('solver', 'space')), may hold values from -6 to 6
- fluid_coef: float32 [128, 256, 512], P(('solver', 'space')), may hold values from 0.25 to 2
- fluid_rhs: float32 [128, 256, 512], P(('solver', 'space')), may hold values from -6 to 6
- wall_start: float32 [3, 8, 128, 256], P(None, None, ('solver', 'space')), may hold values from -4 to 4
- wall_stiff: float32 [8, 128, 256], P(None, ('solver', 'space')), may hold values from 0.5 to 4
- wall_load: float32 [3, 8, 128, 256], P(None, None, ('solver', 'space')), may hold values from -6 to 6
- normals: float32 [3, 32768], P(None, ('solver', 'space')), may hold values from -4 to 4
- fluid_owner: int32 [32768, 1], P(('solver', 'space')), may hold values from 0 to 31; in each aligned block of 1024 rows (0 to 1023, 1024 to 2047, ...) at most 64 rows name the same one
- fluid_cell: int32 [32768], P(('solver', 'space')), may hold values from 0 to 524287
- interface_start: float32 [6, 32768], P(None, ('solver', 'space')), may hold values from -6 to 6
- past_residual: float32 [32, 6, 32768], P(None, None, ('solver', 'space')), may hold values from -4 to 4
- past_output: float32 [32, 6, 32768], P(None, None, ('solver', 'space')), may hold values from -4 to 4
Outputs:
- interface_next: float32 [6, 32768], P(None, ('solver', 'space'))
- pressure: float32 [128, 256, 512], P(('solver', 'space'))
- wall: float32 [3, 8, 128, 256], P(None, None, ('solver', 'space'))
The draws below stay inside these ranges and needn't reach their ends.
Inputs may be any that keep to these rules, and one draw needn't show every extreme that they name: `fluid_owner`: among the 1024 interface points of one device, at most 64 have the same fluid owner.
All inputs are finite; a program needn't handle non-finite values.
Results may differ from the reference program's by a relative error of at most 0.00011.
Values sent between devices are 32-bit elements; how exact they have to be, the bound alone decides.
No kernel may reach another device: no remote copies, remote signals or barrier semaphores. Data moves between devices by JAX's collectives and lax.ppermute only.
A program may use at most 64 MiB of HBM per device.

```python
import math
import jax
import jax.numpy as jnp
import numpy as np
from jax import lax

CX = 4
NY = 256
NZ = 512
SWEEPS = 4
S2 = 256
S3 = 8
KRYLOV = 2
COUPLE = 2
HIST = 32
NX = 128
NS1 = 128
IF_DEV = 1024
NI = 32768
MOST = 64
DEVICES = 32


def place_ends(entries, own_key, least, high):
    place = [jax.random.randint(jax.random.fold_in(own_key, axis), (), 0, length) for axis, length in enumerate(entries.shape)]
    widest = entries.shape.index(max(entries.shape))
    beside = place[:widest] + [(place[widest] + 1) % entries.shape[widest]] + place[widest + 1:]
    return entries.at[tuple(place)].set(least).at[tuple(beside)].set(high)


def level_of(own_key, dims, split, low, largest):
    loudness, own = 1.0, jax.random.fold_in(own_key, 6)
    for position, parts in split:
        draws = jnp.exp(jax.random.uniform(jax.random.fold_in(own, position), (parts,), jnp.float32, low / len(split), largest / len(split)))
        loudness = loudness * jnp.repeat(draws, dims[position] // parts).reshape([-1 if axis == position else 1 for axis in range(len(dims))])
    return loudness


def shared_out(stream_key, own, number, rows, amount, top, reach, lean):
    ranking = jax.random.permutation(stream_key, amount)
    heavy_load, usual = shares(amount, rows * top, reach, lean, True), shares(amount, rows * top, reach, lean, False)
    places = jnp.arange(amount)

    def named(tallies, turn):
        used = int((tallies > 0).sum())
        fixed = max(1, used // 4)
        shifted = fixed + (places - fixed + turn * (used - fixed)) % max(1, amount - fixed)
        return jnp.zeros((amount,), jnp.int32).at[ranking[jnp.where(places < fixed, places, shifted)]].set(jnp.asarray(tallies, jnp.int32))

    tallies = jnp.where(number % 4 == 0, named(heavy_load, number // 4), named(usual, number - number // 4 - 1))
    mixed = jax.random.permutation(jax.random.fold_in(own, 3), amount)
    donor, taker = mixed[0:amount // 2 * 2:2], mixed[1:amount // 2 * 2:2]
    margin = jnp.minimum(tallies[donor] - 1, reach - tallies[taker]) // 2
    margin = jnp.where((donor == ranking[0]) | (taker == ranking[0]) | (tallies[taker] == 0), 0, jnp.maximum(margin, 0))
    shifted = jax.random.randint(jax.random.fold_in(own, 4), (amount // 2,), 0, 1 << 20) % (margin + 1)
    tallies = tallies.at[donor].add(-shifted).at[taker].add(shifted)
    members = jnp.searchsorted(jnp.cumsum(tallies), jnp.arange(rows * top), side="right").astype(jnp.int32)
    grid = members.reshape(top, rows).T
    grid = grid[jax.random.permutation(jax.random.fold_in(own, 1), rows)]
    turn = jax.random.randint(jax.random.fold_in(own, 2), (rows, 1), 0, top)
    return jnp.take_along_axis(grid, (jnp.arange(top)[None, :] + turn) % top, axis=1)


def shares(amount, total, most, skew, full):
    loads = [(1 << 20) // math.isqrt(grade ** skew) + 1 for grade in range(1, amount + 1)]
    largest = most if full else min(most, max(-(-total // amount), total * loads[0] // sum(loads)))
    least = 1 if total - largest >= amount - 1 else 0
    holding, spare = [largest] + [least] * (amount - 1), total - largest - least * (amount - 1)
    while spare > 0:
        free = [i for i in range(1, amount) if holding[i] < largest] or [i for i in range(1, amount) if holding[i] < most]
        pool, left = sum([loads[i] for i in free]), spare
        for i in free:
            extra = min(most - holding[i], max(1, left * loads[i] // pool), spare)
            holding[i] = holding[i] + extra
            spare = spare - extra
    return np.array(holding)


def normal_values(key, shape, width, most, cuts=(), kind=jnp.bfloat16):
    gain = level_of(key, shape, cuts, -0.22, 0.18) if cuts else 1.0
    values = jax.random.normal(key, shape, jnp.float32) * width * gain
    return jnp.minimum(jnp.maximum(values, -most), most).astype(kind)


def setup_inputs(seed: int = 0) -> dict:
    key_list = jax.random.split(jax.random.key(seed), 13)
    pressure_start = normal_values(key_list[0], (NX, NY, NZ), 1.0, 6.0, ((0, 32),), jnp.float32)
    fluid_coef = jnp.clip(0.25 + 1.75 * jax.random.uniform(key_list[1], (NX, NY, NZ), jnp.float32) ** level_of(key_list[1], (NX, NY, NZ), ((0, 32),), -0.2, 0.2), 0.25, 2.0)
    fluid_rhs = normal_values(key_list[2], (NX, NY, NZ), 1.0, 6.0, ((0, 32),), jnp.float32)
    wall_start = normal_values(key_list[3], (3, S3, NS1, S2), 0.5, 4.0, ((2, 32),), jnp.float32)
    wall_stiff = jnp.clip(jnp.exp(math.log(4.0) - 2.0794415 * jax.random.uniform(key_list[4], (S3, NS1, S2), jnp.float32) ** level_of(key_list[4], (S3, NS1, S2), ((1, 32),), -0.2, 0.2)), 0.5, 4.0)
    wall_load = normal_values(key_list[5], (3, S3, NS1, S2), 1.0, 6.0, ((2, 32),), jnp.float32)
    normals = normal_values(key_list[6], (3, NI), 0.6, 4.0, ((1, 32),), jnp.float32)
    fluid_owner_keys = jax.random.split(jax.random.fold_in(key_list[7], 1), NI // IF_DEV)
    fluid_owner_turns = jax.random.permutation(jax.random.fold_in(key_list[7], 3), NI // IF_DEV)
    fluid_owner = jax.vmap(lambda own, number: shared_out(jax.random.fold_in(key_list[7], 2), own, number, IF_DEV, DEVICES, 1, MOST, 2))(fluid_owner_keys, fluid_owner_turns).reshape((NI, 1))
    fluid_cell = place_ends(jax.random.randint(key_list[8], (NI,), 0, CX * NY * NZ), jax.random.fold_in(key_list[8], 1), 0, (CX * NY * NZ) - 1).astype(jnp.int32)
    interface_start = normal_values(key_list[9], (6, NI), 1.0, 6.0, ((1, 32),), jnp.float32)
    past_residual = normal_values(key_list[10], (HIST, 6, NI), 0.5, 4.0, ((2, 32),), jnp.float32)
    past_output = normal_values(key_list[11], (HIST, 6, NI), 0.5, 4.0, ((2, 32),), jnp.float32)
    return {"pressure_start": pressure_start, "fluid_coef": fluid_coef, "fluid_rhs": fluid_rhs, "wall_start": wall_start, "wall_stiff": wall_stiff, "wall_load": wall_load, "normals": normals, "fluid_owner": fluid_owner, "fluid_cell": fluid_cell, "interface_start": interface_start, "past_residual": past_residual, "past_output": past_output}


OMEGA = 0.8
SOURCE_GAIN = 4.0
RIDGE = 0.1
TINY = 1e-06

def fluid_sweep(field, rhs, diag):
    padded = jnp.pad(field, 1)
    beside = padded[2:, 1:-1, 1:-1] + padded[:-2, 1:-1, 1:-1]
    beside = beside + padded[1:-1, 2:, 1:-1] + padded[1:-1, :-2, 1:-1]
    beside = beside + padded[1:-1, 1:-1, 2:] + padded[1:-1, 1:-1, :-2]
    return (1.0 - OMEGA) * field + OMEGA * (rhs + beside) / diag

def wall_apply(field, stiff):
    padded = jnp.pad(field, ((0, 0), (1, 1), (1, 1), (0, 0)))
    beside = padded[:, 2:, 1:-1] + padded[:, :-2, 1:-1] + padded[:, 1:-1, 2:] + padded[:, 1:-1, :-2]
    beside = beside + jnp.roll(field, 1, 3) + jnp.roll(field, -1, 3)
    return (6.0 + stiff) * field - beside

def wall_solve(force, stiff):
    solution = jnp.zeros_like(force)
    residual = force
    direction = force
    norm_now = jnp.sum(residual * residual)
    for step in range(KRYLOV):
        image = wall_apply(direction, stiff)
        alpha = norm_now / jnp.sum(direction * image)
        solution = solution + alpha * direction
        residual = residual - alpha * image
        if step + 1 < KRYLOV:
            norm_next = jnp.sum(residual * residual)
            direction = residual + norm_next / norm_now * direction
            norm_now = norm_next
    return solution

def reference(pressure_start, fluid_coef, fluid_rhs, wall_start, wall_stiff, wall_load, normals, fluid_owner, fluid_cell, interface_start, past_residual, past_output):
    highest = lax.Precision.HIGHEST
    where = (fluid_owner[:, 0] * (CX * NY * NZ) + fluid_cell).astype(jnp.int32)
    diag = 6.0 + fluid_coef
    base = wall_load - wall_apply(wall_start, wall_stiff)
    state = interface_start
    pressure = pressure_start
    stack_res = past_residual
    stack_out = past_output
    last_res = state
    last_out = state
    wall = wall_start
    for turn in range(COUPLE):
        displace = state[0:3]
        traction = state[3:6]
        flux = SOURCE_GAIN * jnp.sum(normals * displace, axis=0)
        source = jnp.zeros((NX * NY * NZ,), jnp.float32).at[where].add(flux).reshape(NX, NY, NZ)
        rhs = fluid_rhs + source
        for sweep in range(SWEEPS):
            pressure = fluid_sweep(pressure, rhs, diag)
        fluid_out = -pressure.reshape(-1)[where][None, :] * normals
        force = base.at[:, 0].add(traction.reshape(3, NS1, S2))
        wall = wall_start + wall_solve(force, wall_stiff)
        solid_out = wall[:, 0].reshape(3, NI)
        output = jnp.concatenate([solid_out, fluid_out], axis=0)
        resid = output - state
        if turn > 0:
            stack_res = jnp.concatenate([(resid - last_res)[None], stack_res[:-1]], axis=0)
            stack_out = jnp.concatenate([(output - last_out)[None], stack_out[:-1]], axis=0)
        last_res = resid
        last_out = output
        gram = jnp.einsum('aci,bci->ab', stack_res, stack_res, precision=highest)
        proj = jnp.einsum('aci,ci->a', stack_res, resid, precision=highest)
        ridge = RIDGE * jnp.trace(gram) / HIST + TINY
        factor = jnp.linalg.cholesky(gram + ridge * jnp.eye(HIST, dtype=jnp.float32))
        half = lax.linalg.triangular_solve(factor, proj[:, None], left_side=True, lower=True)
        coeffs = -lax.linalg.triangular_solve(factor, half, left_side=True, lower=True, transpose_a=True)[:, 0]
        state = output + jnp.einsum('a,aci->ci', coeffs, stack_out, precision=highest)
    return (state, pressure, wall)
```

```python
import functools

import jax
import jax.numpy as jnp
from jax import lax
from jax.experimental import pallas as pl
from jax.experimental.pallas import tpu as pltpu
from jax.sharding import PartitionSpec as P

SWEEPS = 4
KRYLOV = 2
COUPLE = 2

OMEGA = 0.8
SOURCE_GAIN = 4.0
RIDGE = 0.1
TINY = 1e-06

AXES = ("solver", "space")
LANES = 128
SUB = 8
HIGHEST = lax.Precision.HIGHEST
F32 = jnp.float32


def vmem():
    return pl.BlockSpec(memory_space=pltpu.VMEM)


def smem():
    return pl.BlockSpec(memory_space=pltpu.SMEM)


def call(kernel, outs, ins, scratch=(), limit=16, name=None):
    return pl.pallas_call(
        kernel,
        out_shape=[jax.ShapeDtypeStruct(shape, dtype) for shape, dtype in outs],
        in_specs=ins,
        out_specs=[vmem() for _ in outs],
        scratch_shapes=list(scratch),
        compiler_params=pltpu.CompilerParams(vmem_limit_bytes=limit * 1024 * 1024),
        name=name,
    )


def dot(a, b, dims):
    return lax.dot_general(a, b, (dims, ((), ())), precision=HIGHEST, preferred_element_type=F32)


def iota(shape, dim):
    return lax.broadcasted_iota(jnp.int32, shape, dim)


def exchange(send):
    return lax.all_to_all(send, AXES, split_axis=0, concat_axis=0, tiled=True)


def pairs():
    count = lax.axis_size(AXES)
    near = [(i, i ^ 1) for i in range(count)]
    up = [(i, i + 1) for i in range(1, count - 1, 2)]
    return near, up + [(target, source) for source, target in up]


def swap(near, far):
    first, second = pairs()
    return lax.ppermute(near, AXES, first), lax.ppermute(far, AXES, second)


def onehots(owner, rank, devices, most):
    points = owner.shape[1]
    named = (owner == iota((devices, points), 0)).astype(F32)
    placed = (rank == iota((most, points), 0)).astype(F32)
    return named, placed


def flux_of(normals, state):
    product = normals * state[0:3]
    return SOURCE_GAIN * (product[0:1] + product[1:2] + product[2:3])


def route_kernel(devices, most, owner_ref, cell_ref, normals_ref, state_ref, send_ref, rank_ref):
    points = owner_ref.shape[1]
    owner = owner_ref[...]
    named = (owner == iota((devices, points), 0)).astype(F32)
    blocks = [named[:, i * LANES : (i + 1) * LANES] for i in range(points // LANES)]
    earlier = (iota((LANES, LANES), 0) < iota((LANES, LANES), 1)).astype(jnp.bfloat16)
    base = jnp.zeros((devices, 1), F32)
    for i, block in enumerate(blocks):
        ahead = jnp.dot(block.astype(jnp.bfloat16), earlier, preferred_element_type=F32) + base
        rank_ref[:, i * LANES : (i + 1) * LANES] = jnp.sum(ahead * block, axis=0, keepdims=True).astype(jnp.int32)
        base = base + jnp.sum(block, axis=1, keepdims=True)
    placed = (rank_ref[...] == iota((most, points), 0)).astype(F32)
    flux = flux_of(normals_ref[...], state_ref[...])
    marks = (cell_ref[...] + 1).astype(F32)
    send_ref[...] = jnp.zeros_like(send_ref)
    send_ref[:, 0:most] = dot(named, placed * marks, ((1,), (1,)))
    send_ref[:, most : 2 * most] = dot(named, placed * flux, ((1,), (1,)))


def tiled_place(cell, depth):
    across = depth // LANES
    row, along = cell // depth, cell % depth
    tile = (row // SUB) * across + along // LANES
    return (tile * SUB + row % SUB) * LANES + along % LANES


def scatter_kernel(most, first, code_ref, value_ref, rhs_ref, out_ref, *grids):
    across = rhs_ref.shape[1] // LANES
    count = len(grids)
    place = iota((SUB, LANES), 0) * LANES + iota((SUB, LANES), 1)
    area = SUB * LANES
    fill = 8

    def clear(step, carry):
        for grid in grids:
            grid[pl.ds(step * fill, fill)] = jnp.zeros((fill, SUB, LANES), F32)
        return carry

    lax.fori_loop(0, grids[0].shape[0] // fill, clear, 0)
    devices = code_ref.shape[0]
    part = devices // count

    def outer(d, carry):
        for slot in range(most):
            codes = [code_ref[g * part + d, slot] for g in range(count)]
            tiles = [lax.shift_right_logical(code, area.bit_length() - 1) for code in codes]
            added = [
                grid[tile] + jnp.where(place == (code & (area - 1)), value_ref[g * part + d, first + slot], 0.0)
                for g, (grid, tile, code) in enumerate(zip(grids, tiles, codes))
            ]
            for grid, tile, new in zip(grids, tiles, added):
                grid[tile] = new
        return carry

    lax.fori_loop(0, part, outer, 0)

    def gather_up(step, carry):
        spot = pl.ds(pl.multiple_of(step * SUB, SUB), SUB)
        for t in range(across):
            total = rhs_ref[spot, t * LANES : (t + 1) * LANES]
            for grid in grids:
                total = total + grid[step * across + t]
            out_ref[spot, t * LANES : (t + 1) * LANES] = total
        return carry

    lax.fori_loop(0, out_ref.shape[0] // SUB, gather_up, 0)


def gather_kernel(most, code_ref, field_ref, extra_ref, out_ref, lines_ref, flat_ref):
    width = field_ref.shape[1]
    across = width // LANES

    def flatten(j, carry):
        for t in range(across):
            to = pl.ds(pl.multiple_of((j * across + t) * SUB, SUB), SUB)
            flat_ref[to, :] = field_ref[pl.ds(pl.multiple_of(j * SUB, SUB), SUB), t * LANES : (t + 1) * LANES]
        return carry

    lax.fori_loop(0, field_ref.shape[0] // SUB, flatten, 0)
    devices = code_ref.shape[0]
    lane = iota((1, LANES), 1)
    unroll = 16

    def outer(d, carry):
        base = pl.multiple_of(d * most, SUB)
        for low in range(0, most, unroll):
            found = []
            for k in range(min(unroll, most - low)):
                code = code_ref[d, low + k]
                line = flat_ref[pl.ds(lax.shift_right_logical(code, LANES.bit_length() - 1), 1), :]
                found.append(jnp.where(lane == (code & (LANES - 1)), line, 0.0))
            for k, line in enumerate(found):
                lines_ref[pl.ds(base + (low + k), 1), :] = line
        return carry

    lax.fori_loop(0, devices, outer, 0)
    ones = jnp.ones((SUB, LANES), F32)
    found = dot(ones, lines_ref[...], ((1,), (1,)))
    out_ref[...] = jnp.zeros_like(out_ref)
    out_ref[:, most : most + 2] = jnp.broadcast_to(extra_ref[:, 0:2], (devices, 2))
    for d in range(devices):
        out_ref[d : d + 1, 0:most] = found[0:1, d * most : (d + 1) * most]


def sweep_kernel(rows, me_ref, field_ref, near_ref, far_ref, rhs_ref, scale_ref, out_ref, *sends):
    wide, depth = near_ref.shape
    sub = iota((SUB, depth), 0)
    lane = iota((SUB, depth), 1)
    even = (me_ref[0] & 1) == 0
    blocks = wide // SUB
    unroll = 2

    def block(j):
        y = pl.multiple_of(j * SUB, SUB)
        above = pl.multiple_of(jnp.maximum(j - 1, 0) * SUB, SUB)
        below = pl.multiple_of(jnp.minimum(j + 1, blocks - 1) * SUB, SUB)
        top = (sub == 0) & (j == 0)
        bottom = (sub == SUB - 1) & (j == blocks - 1)
        near, far = near_ref[pl.ds(y, SUB), :], far_ref[pl.ds(y, SUB), :]
        low, high = jnp.where(even, far, near), jnp.where(even, near, far)
        tiles = [field_ref[pl.ds(x * wide + y, SUB), :] for x in range(rows)]
        edge = []
        for x, here in enumerate(tiles):
            spot = pl.ds(x * wide + y, SUB)
            over = field_ref[pl.ds(x * wide + above, SUB), :]
            under = field_ref[pl.ds(x * wide + below, SUB), :]
            beside = (low if x == 0 else tiles[x - 1]) + (high if x == rows - 1 else tiles[x + 1])
            ahead = pltpu.roll(jnp.where(sub == SUB - 1, over, here), 1, 0)
            behind = pltpu.roll(jnp.where(sub == 0, under, here), SUB - 1, 0)
            beside = beside + jnp.where(top, 0.0, ahead)
            beside = beside + jnp.where(bottom, 0.0, behind)
            beside = beside + jnp.where(lane == 0, 0.0, pltpu.roll(here, 1, 1))
            beside = beside + jnp.where(lane == depth - 1, 0.0, pltpu.roll(here, depth - 1, 1))
            new = (1.0 - OMEGA) * here + (rhs_ref[spot, :] + beside) * scale_ref[spot, :]
            out_ref[spot, :] = new
            if x in (0, rows - 1):
                edge.append(new)
        if sends:
            sends[0][pl.ds(y, SUB), :] = jnp.where(even, edge[1], edge[0])
            sends[1][pl.ds(y, SUB), :] = jnp.where(even, edge[0], edge[1])

    def step(j, carry):
        for k in range(unroll):
            block(j * unroll + k)
        return carry

    lax.fori_loop(0, blocks // unroll, step, 0)


def stencil(field, stiff, layers, edge=None):
    sub = iota(field[0].shape, 0)
    turns = field[0].shape[1]
    out = []
    for index, here in enumerate(field):
        layer = index % layers
        before, after = pltpu.roll(here, 1, 0), pltpu.roll(here, SUB - 1, 0)
        if edge is not None:
            before = jnp.where(sub == 0, edge[index][0], before)
            after = jnp.where(sub == SUB - 1, edge[index][1], after)
        beside = before + after + pltpu.roll(here, 1, 1) + pltpu.roll(here, turns - 1, 1)
        if layer > 0:
            beside = beside + field[index - 1]
        if layer < layers - 1:
            beside = beside + field[index + 1]
        out.append((6.0 + stiff[layer]) * here - beside)
    return out


def inner(left, right, own):
    total = jnp.zeros_like(left[0])
    for a, b in zip(left, right):
        total = total + a * b
    return jnp.sum(jnp.where(own, total, 0.0), keepdims=True)


def wall_parts(force, stiff, layers, lead, valid, own, force_ref, image_ref, twice_ref):
    force = [jnp.where(valid, tile, 0.0) for tile in force]
    image = [jnp.where(valid, tile, 0.0) for tile in stencil(force, stiff, layers)]
    twice = stencil(image, stiff, layers)
    for index in range(len(force)):
        force_ref[index] = force[index]
        image_ref[index] = image[index]
        twice_ref[index] = twice[index]
    return inner(force, force, own), inner(force, image, own)


def row_masks(me, devices, rows, shape):
    lead = (SUB - rows) // 2
    sub = iota(shape, 0)
    valid = ((sub >= lead) | (me > 0)) & ((sub < lead + rows) | (me < devices - 1))
    own = (sub >= lead) & (sub < lead + rows)
    return valid, own


def two_lanes(first, second, lanes):
    lane = iota((1, lanes), 1)
    return jnp.where(lane == 0, first, jnp.where(lane == 1, second, 0.0))


def wall_first_kernel(devices, layers, me_ref, own_ref, near_ref, far_ref, past_ref,
                      send_ref, base_ref, stiff_ref, force_ref, image_ref, twice_ref, wide_ref):
    count, rows, turns = own_ref.shape
    lead = (SUB - rows) // 2
    even = (me_ref[0] & 1) == 0
    wide_ref[:, 0:lead, :] = jnp.where(even, far_ref[:, rows - lead : rows, :], near_ref[:, rows - lead : rows, :])
    wide_ref[:, lead : lead + rows, :] = own_ref[...]
    wide_ref[:, lead + rows : SUB, :] = jnp.where(even, near_ref[:, 0:lead, :], far_ref[:, 0:lead, :])
    tiles = 3 * layers
    start = [wide_ref[i] for i in range(tiles)]
    outer = slice(rows - lead - 1, rows - lead)
    edge = [
        (jnp.where(even, far_ref[i, outer, :], near_ref[i, outer, :]),
         jnp.where(even, near_ref[i, lead : lead + 1, :], far_ref[i, lead : lead + 1, :]))
        for i in range(tiles)
    ]
    stiff = [wide_ref[2 * tiles + i] for i in range(layers)]
    for i in range(layers):
        stiff_ref[i] = stiff[i]
    applied = stencil(start, stiff, layers, edge)
    for i in range(tiles):
        base_ref[i] = wide_ref[tiles + i] - applied[i]
    valid, own = row_masks(me_ref[0], devices, rows, (SUB, turns))
    force = [base_ref[i] for i in range(tiles)]
    for c in range(3):
        force[c * layers] = force[c * layers] + wide_ref[2 * tiles + layers + c]
    square, product = wall_parts(force, stiff, layers, lead, valid, own, force_ref, image_ref, twice_ref)
    history = past_ref.shape[1]
    gram = jnp.zeros((history, history), F32)
    for c in range(past_ref.shape[0]):
        gram = gram + dot(past_ref[c], past_ref[c], ((1,), (1,)))
    send_ref[:, 0:LANES] = jnp.broadcast_to(two_lanes(square, product, LANES), (devices, LANES))
    for a in range(history):
        left = LANES + a * history
        send_ref[:, left : left + history] = jnp.broadcast_to(gram[a : a + 1, :], (devices, history))


def wall_next_kernel(devices, layers, rows, me_ref, got_ref, state_ref, base_ref, stiff_ref,
                     send_ref, force_ref, image_ref, twice_ref, pull_ref):
    tiles, _, turns = base_ref.shape
    lead = (SUB - rows) // 2
    me = me_ref[0]
    before, after = jnp.maximum(me - 1, 0), jnp.minimum(me + 1, devices - 1)
    reach = lead * turns
    for c in range(3):
        for s in range(rows):
            pull_ref[c, lead + s : lead + s + 1, :] = state_ref[3 + c : 4 + c, s * turns : (s + 1) * turns]
        for s in range(lead):
            spot = pl.ds(c * reach + s * turns, turns)
            pull_ref[c, s : s + 1, :] = got_ref[pl.ds(before, 1), spot]
            pull_ref[c, lead + rows + s : lead + rows + s + 1, :] = got_ref[pl.ds(after, 1), spot]
    valid, own = row_masks(me, devices, rows, (SUB, turns))
    force = [base_ref[i] for i in range(tiles)]
    for c in range(3):
        force[c * layers] = force[c * layers] + pull_ref[c]
    stiff = [stiff_ref[i] for i in range(layers)]
    square, product = wall_parts(force, stiff, layers, lead, valid, own, force_ref, image_ref, twice_ref)
    send_ref[...] = jnp.broadcast_to(two_lanes(square, product, LANES), (devices, LANES))


def summed(got_ref, lanes):
    return jnp.sum(got_ref[:, 0:lanes], axis=0, keepdims=True)


def wall_second_kernel(rows, got_ref, force_ref, image_ref, twice_ref, send_ref):
    total = summed(got_ref, LANES)
    alpha = total[:, 0:1] / total[:, 1:2]
    shape = force_ref.shape[1:]
    lead = (SUB - rows) // 2
    sub = iota(shape, 0)
    own = (sub >= lead) & (sub < lead + rows)
    square = jnp.zeros(shape, F32)
    product = jnp.zeros(shape, F32)
    for i in range(force_ref.shape[0]):
        residual = force_ref[i] - alpha * image_ref[i]
        image = image_ref[i] - alpha * twice_ref[i]
        square = square + residual * residual
        product = product + residual * image
    square = jnp.sum(jnp.where(own, square, 0.0), keepdims=True)
    product = jnp.sum(jnp.where(own, product, 0.0), keepdims=True)
    send_ref[...] = two_lanes(square, product, LANES)


def wall_last_kernel(layers, rows, most, one_ref, two_ref, force_ref, image_ref, start_ref, wall_ref, solid_ref):
    one = summed(one_ref, LANES)
    two = jnp.sum(two_ref[:, most : most + 2], axis=0, keepdims=True)
    norm, alpha = one[:, 0:1], one[:, 0:1] / one[:, 1:2]
    newer = two[:, 0:1]
    ratio = newer / norm
    beta = newer / (two[:, 1:2] - ratio * newer / alpha)
    turns = force_ref.shape[2]
    lead = (SUB - rows) // 2
    for i in range(force_ref.shape[0]):
        c, layer = i // layers, i % layers
        force = force_ref[i]
        residual = force - alpha * image_ref[i]
        moved = alpha * force + beta * (residual + ratio * force)
        wall = start_ref[c, layer] + moved[lead : lead + rows, :]
        wall_ref[c, layer] = wall
        if layer == 0:
            for s in range(rows):
                solid_ref[c : c + 1, s * turns : (s + 1) * turns] = wall[s : s + 1, :]


def returned_kernel(devices, most, turn, got_ref, owner_ref, rank_ref, normals_ref, state_ref, solid_ref, past_ref, *rest):
    if turn == 0:
        output_ref, resid_ref, send_ref = rest
    else:
        last_ref, output_ref, resid_ref, send_ref = rest
    named, placed = onehots(owner_ref[...], rank_ref[...], devices, most)
    spread = dot(got_ref[:, 0:most], named, ((0,), (0,)))
    sampled = jnp.sum(spread * placed, axis=0, keepdims=True)
    output_ref[0:3, :] = solid_ref[...]
    output_ref[3:6, :] = -sampled * normals_ref[...]
    resid_ref[...] = output_ref[...] - state_ref[...]
    history = past_ref.shape[1]
    points = state_ref.shape[1]
    sub = iota((SUB, points), 0)
    parts = jnp.zeros((SUB, history), F32)
    newest = jnp.zeros((SUB, SUB), F32)
    for c in range(6):
        resid = resid_ref[c : c + 1, :]
        pair = jnp.where(sub == 0, resid, 0.0)
        if turn > 0:
            pair = jnp.where(sub == 1, resid - last_ref[c : c + 1, :], pair)
            newest = newest + dot(pair, pair, ((1,), (1,)))
        parts = parts + dot(pair, past_ref[c], ((1,), (1,)))
    send_ref[...] = jnp.zeros_like(send_ref)
    send_ref[:, 0:history] = jnp.broadcast_to(parts[0:1, :], (devices, history))
    if turn > 0:
        send_ref[:, history : 2 * history] = jnp.broadcast_to(parts[1:2, :], (devices, history))
        send_ref[:, 2 * history : 2 * history + 2] = jnp.broadcast_to(newest[1:2, 0:2], (devices, 2))


def coefficients(turn, history, got_ref, gram_ref, work_ref):
    total = summed(got_ref, got_ref.shape[1])
    flat = summed(gram_ref, gram_ref.shape[1])
    work_ref[...] = jnp.zeros_like(work_ref)
    for a in range(history):
        left = LANES + a * history
        work_ref[a : a + 1, 0:history] = flat[:, left : left + history]
    work_ref[history : history + 1, 0:history] = total[:, 0:history]
    shape = work_ref.shape
    sub, lane = iota(shape, 0), iota(shape, 1)
    if turn > 0:
        swap = history - 1
        fresh = total[:, history : 2 * history]
        square = total[:, 2 * history + 1 : 2 * history + 2]
        along = total[:, 2 * history : 2 * history + 1]
        edge = iota((1, history), 1) == swap
        work_ref[swap : swap + 1, 0:history] = jnp.where(edge, square, fresh)
        work_ref[history : history + 1, 0:history] = jnp.where(edge, along, total[:, 0:history])
        line = work_ref[swap : swap + 1, :]
        column = jnp.sum(jnp.where(sub == lane, line, 0.0), axis=1, keepdims=True)
        table = work_ref[...]
        table = jnp.where((lane == swap) & (sub < history), column, table)
    else:
        table = work_ref[...]
    diagonal = (sub == lane) & (sub < history)
    trace = jnp.sum(jnp.where(diagonal, table, 0.0), keepdims=True)
    ridge = RIDGE * trace / history + TINY
    table = jnp.where(diagonal, table + ridge, table)
    table = jnp.where((lane == sub + history) & (sub < history), 1.0, table)
    for k in range(history):
        line = table[k : k + 1, :]
        column = jnp.where(sub[:, 0:1] > k, table[:, k : k + 1], 0.0)
        table = table - (column / line[:, k : k + 1]) * line
    return table[history : history + 1, history : 2 * history]


def update_kernel(devices, most, turn, got_ref, gram_ref, output_ref, past_ref, *rest):
    history = past_ref.shape[1]
    if turn == 0:
        me_ref, owner_ref, rank_ref, normals_ref, next_ref, send_ref, work_ref = rest
    else:
        last_ref, next_ref, work_ref = rest
    coeffs = coefficients(turn, history, got_ref, gram_ref, work_ref)
    rows = jnp.broadcast_to(coeffs, (SUB, history))
    swap = history - 1
    if turn > 0:
        newest = coeffs[:, swap:history]
        rows = jnp.where(iota(rows.shape, 1) == swap, 0.0, rows)
    for c in range(6):
        moved = dot(rows, past_ref[c], ((1,), (0,)))[0:1, :]
        here = output_ref[c : c + 1, :]
        if turn > 0:
            moved = moved + newest * (here - last_ref[c : c + 1, :])
        next_ref[c : c + 1, :] = here + moved
    if turn == 0:
        me = me_ref[0]
        points = output_ref.shape[1]
        half = (send_ref.shape[1] - LANES) // 3
        named, placed = onehots(owner_ref[...], rank_ref[...], devices, most)
        flux = flux_of(normals_ref[...], next_ref[...])
        send_ref[...] = jnp.zeros_like(send_ref)
        left = 3 * half
        send_ref[:, left : left + most] = dot(named, placed * flux, ((1,), (1,)))
        for c in range(3):
            tract = next_ref[3 + c : 4 + c, :]
            spot = pl.ds(c * half, half)

            @pl.when(me > 0)
            def _():
                send_ref[pl.ds(me - 1, 1), spot] = tract[:, 0:half]

            @pl.when(me < devices - 1)
            def _():
                send_ref[pl.ds(me + 1, 1), spot] = tract[:, points - half : points]


def local(
    pressure_start,
    fluid_coef,
    fluid_rhs,
    wall_start,
    wall_stiff,
    wall_load,
    normals,
    fluid_owner,
    fluid_cell,
    interface_start,
    past_residual,
    past_output,
):
    devices = lax.axis_size(AXES)
    me = lax.axis_index(AXES).astype(jnp.int32).reshape(1)
    rows, wide, depth = pressure_start.shape
    points = fluid_cell.shape[0]
    most = max(2, 2 * points // devices)
    history = past_residual.shape[0]
    layers, wall_rows, turns = wall_stiff.shape
    flat = (rows * wide, depth)
    plane = (wide, depth)
    lead = (SUB - wall_rows) // 2
    tiles = 3 * layers
    tile = (tiles, SUB, turns)
    slots = LANES * -(-2 * most // LANES)

    owner = fluid_owner.reshape(1, points)
    field = pressure_start.reshape(flat)
    low, high = field[0:wide], field[flat[0] - wide :]
    even = (me[0] & 1) == 0
    near, far = swap(jnp.where(even, high, low), jnp.where(even, low, high))

    send, rank = call(
        functools.partial(route_kernel, devices, most),
        [((devices, slots), F32), ((1, points), jnp.int32)],
        [vmem()] * 4, name="route",
    )(owner, fluid_cell.reshape(1, points), normals, interface_start)
    got = exchange(send)
    cells = tiled_place(jnp.maximum(got[:, 0:most].astype(jnp.int32) - 1, 0), depth)
    flux, spot = got, most

    pack = jnp.concatenate(
        [
            wall_start.reshape(tiles, wall_rows, turns),
            wall_load.reshape(tiles, wall_rows, turns),
            wall_stiff,
            interface_start[3:6].reshape(3, wall_rows, turns),
        ],
        axis=0,
    )
    pack_near, pack_far = swap(pack, pack)
    past_r = jnp.transpose(past_residual, (1, 0, 2))
    past_w = jnp.transpose(past_output, (1, 0, 2))
    scale = (OMEGA / (6.0 + fluid_coef)).reshape(flat)
    rhs = fluid_rhs.reshape(flat)

    sums, base, stiff, force, image, twice = call(
        functools.partial(wall_first_kernel, devices, layers),
        [((devices, LANES + history * history), F32), (tile, F32), ((layers, SUB, turns), F32), (tile, F32), (tile, F32), (tile, F32)],
        [smem()] + [vmem()] * 4,
        [pltpu.VMEM((pack.shape[0], SUB, turns), F32)], limit=6, name="wall_first",
    )(me, pack, pack_near, pack_far, past_r)
    one = exchange(sums)
    grams = one

    state = interface_start
    output = resid = wall = None
    for turn in range(COUPLE):
        source = call(
            functools.partial(scatter_kernel, most, spot),
            [(flat, F32)],
            [smem(), smem(), vmem()],
            [pltpu.VMEM((flat[0] * depth // (SUB * LANES), SUB, LANES), F32)] * SUB, limit=18, name="scatter",
        )(cells, flux, rhs)[0]
        for sweep in range(SWEEPS):
            if turn > 0 or sweep > 0:
                near, far = swap(*ends)
            closing = turn + 1 == COUPLE and sweep + 1 == SWEEPS
            field, *ends = call(
                functools.partial(sweep_kernel, rows),
                [(flat, F32)] + [(plane, F32)] * (0 if closing else 2), [smem()] + [vmem()] * 5, limit=12, name="sweep",
            )(me, field, near, far, source, scale)
            if sweep == 1 and turn > 0:
                sums, force, image, twice = call(
                    functools.partial(wall_next_kernel, devices, layers, wall_rows),
                    [((devices, LANES), F32), (tile, F32), (tile, F32), (tile, F32)],
                    [smem()] + [vmem()] * 4,
                    [pltpu.VMEM((3, SUB, turns), F32)], limit=2, name="wall_next",
                )(me, pulls, state, base, stiff)
                one = exchange(sums)
        sums = call(
            functools.partial(wall_second_kernel, wall_rows),
            [((1, LANES), F32)], [vmem()] * 4, limit=2, name="wall_second",
        )(one, force, image, twice)[0]
        sampled = call(
            functools.partial(gather_kernel, most),
            [((devices, LANES * -(-(most + 2) // LANES)), F32)],
            [smem(), vmem(), vmem()],
            [pltpu.VMEM((devices * most, LANES), F32), pltpu.VMEM((flat[0] * depth // LANES, LANES), F32)], limit=6, name="gather",
        )(cells, field, sums)[0]
        back = exchange(sampled)
        wall, solid = call(
            functools.partial(wall_last_kernel, layers, wall_rows, most),
            [(wall_start.shape, F32), ((3, points), F32)], [vmem()] * 5, limit=2, name="wall_last",
        )(one, back, force, image, wall_start)
        last_args = () if turn == 0 else (resid,)
        before = output
        output, resid, sums = call(
            functools.partial(returned_kernel, devices, most, turn),
            [((6, points), F32), ((6, points), F32), ((devices, LANES * -(-(2 * history + 2) // LANES)), F32)],
            [vmem()] * (7 + len(last_args)), limit=4, name="returned",
        )(back, owner, rank, normals, state, solid, past_r, *last_args)
        total = exchange(sums)
        work = [pltpu.VMEM((SUB * -(-(history + 1) // SUB), LANES * -(-2 * history // LANES)), F32)]
        if turn + 1 < COUPLE:
            state, send = call(
                functools.partial(update_kernel, devices, most, 0),
                [((6, points), F32), ((devices, 3 * lead * turns + LANES * -(-most // LANES)), F32)],
                [vmem()] * 4 + [smem()] + [vmem()] * 3, work, limit=4, name="update",
            )(total, grams, output, past_w, me, owner, rank, normals)
            pulls = exchange(send)
            flux, spot = pulls[:, 3 * lead * turns :], 0
        else:
            state = call(
                functools.partial(update_kernel, devices, most, 1),
                [((6, points), F32)], [vmem()] * 5, work, limit=4, name="finish",
            )(total, grams, output, past_w, before)[0]
    return (state, field.reshape(pressure_start.shape), wall)


def solution(mesh):
    placed = (
        P(("solver", "space"), None, None),
        P(("solver", "space"), None, None),
        P(("solver", "space"), None, None),
        P(None, None, ("solver", "space"), None),
        P(None, ("solver", "space"), None),
        P(None, None, ("solver", "space"), None),
        P(None, ("solver", "space")),
        P(("solver", "space"), None),
        P(("solver", "space")),
        P(None, ("solver", "space")),
        P(None, None, ("solver", "space")),
        P(None, None, ("solver", "space")),
    )
    return jax.shard_map(
        local,
        mesh=mesh,
        in_specs=placed,
        out_specs=(
            P(None, ("solver", "space")),
            P(("solver", "space"), None, None),
            P(None, None, ("solver", "space"), None),
        ),
        check_vma=False,
    )
```

```python
import functools

import jax
import jax.numpy as jnp
from jax import lax
from jax.experimental import pallas as pl
from jax.experimental.pallas import tpu as pltpu
from jax.sharding import PartitionSpec as P


SWEEPS = 4
COUPLE = 2

OMEGA = 0.8
SOURCE_GAIN = 4.0
RIDGE = 0.1
TINY = 1e-06

AXES = ("solver", "space")
LANES = 128
GRIDS = 4
SUB = 8
HIGHEST = lax.Precision.HIGHEST
F32 = jnp.float32


def vmem():
    return pl.BlockSpec(memory_space=pltpu.VMEM)


def smem():
    return pl.BlockSpec(memory_space=pltpu.SMEM)


def call(kernel, outs, ins, scratch=(), limit=16):
    return pl.pallas_call(
        kernel,
        out_shape=[jax.ShapeDtypeStruct(shape, dtype) for shape, dtype in outs],
        in_specs=ins,
        out_specs=[vmem() for _ in outs],
        scratch_shapes=list(scratch),
        compiler_params=pltpu.CompilerParams(vmem_limit_bytes=limit * 1024 * 1024),
    )


def dot(a, b, dims):
    return lax.dot_general(a, b, (dims, ((), ())), precision=HIGHEST, preferred_element_type=F32)


def iota(shape, dim):
    return lax.broadcasted_iota(jnp.int32, shape, dim)


def exchange(send):
    return lax.all_to_all(send, AXES, split_axis=0, concat_axis=0, tiled=True)


def tie(*values):
    return lax.optimization_barrier(values)


def pairs():
    count = lax.axis_size(AXES)
    near = [(i, i ^ 1) for i in range(count)]
    up = [(i, i + 1) for i in range(1, count - 1, 2)]
    return near, up + [(target, source) for source, target in up]


def swap(near, far):
    first, second = pairs()
    return lax.ppermute(near, AXES, first), lax.ppermute(far, AXES, second)


def onehots(owner, rank, devices, most):
    points = owner.shape[1]
    named = (owner == iota((devices, points), 0)).astype(F32)
    placed = (rank == iota((most, points), 0)).astype(F32)
    return named, placed


def flux_of(normals, state):
    product = normals * state[0:3]
    return SOURCE_GAIN * (product[0:1] + product[1:2] + product[2:3])


def route_kernel(devices, most, owner_ref, cell_ref, normals_ref, state_ref, send_ref, rank_ref):
    points = owner_ref.shape[1]
    owner = owner_ref[...]
    named = (owner == iota((devices, points), 0)).astype(F32)
    blocks = [named[:, i * LANES : (i + 1) * LANES] for i in range(points // LANES)]
    earlier = (iota((LANES, LANES), 0) < iota((LANES, LANES), 1)).astype(jnp.bfloat16)
    base = jnp.zeros((devices, 1), F32)
    for i, block in enumerate(blocks):
        ahead = jnp.dot(block.astype(jnp.bfloat16), earlier, preferred_element_type=F32) + base
        rank_ref[:, i * LANES : (i + 1) * LANES] = jnp.sum(ahead * block, axis=0, keepdims=True).astype(jnp.int32)
        base = base + jnp.sum(block, axis=1, keepdims=True)
    placed = (rank_ref[...] == iota((most, points), 0)).astype(F32)
    flux = flux_of(normals_ref[...], state_ref[...])
    marks = (cell_ref[...] + 1).astype(F32)
    send_ref[...] = jnp.zeros_like(send_ref)
    send_ref[:, 0:most] = dot(named, placed * marks, ((1,), (1,)))
    send_ref[:, most : 2 * most] = dot(named, placed * flux, ((1,), (1,)))


def tiled_place(cell, depth):
    across = depth // LANES
    row, along = cell // depth, cell % depth
    tile = (row // SUB) * across + along // LANES
    return (tile * SUB + row % SUB) * LANES + along % LANES


def scatter_cells(most, first, code_ref, value_ref, grids):
    count = len(grids)
    place = iota((SUB, LANES), 0) * LANES + iota((SUB, LANES), 1)
    area = SUB * LANES
    fill = 8

    def clear(step, carry):
        for grid in grids:
            grid[pl.ds(step * fill, fill)] = jnp.zeros((fill, SUB, LANES), F32)
        return carry

    lax.fori_loop(0, grids[0].shape[0] // fill, clear, 0)
    part = code_ref.shape[0] // count

    def outer(d, carry):
        for slot in range(most):
            codes = [code_ref[g * part + d, slot] for g in range(count)]
            tiles = [lax.shift_right_logical(code, area.bit_length() - 1) for code in codes]
            added = [
                grid[tile] + jnp.where(place == (code & (area - 1)), value_ref[g * part + d, first + slot], 0.0)
                for g, (grid, tile, code) in enumerate(zip(grids, tiles, codes))
            ]
            for grid, tile, new in zip(grids, tiles, added):
                grid[tile] = new
        return carry

    lax.fori_loop(0, part, outer, 0)


def gather_cells(most, code_ref, flat_ref, extra_ref, out_ref, lines_ref):
    devices = code_ref.shape[0]
    lane = iota((1, LANES), 1)
    unroll = 16

    def outer(d, carry):
        base = pl.multiple_of(d * most, SUB)
        for low in range(0, most, unroll):
            found = []
            for k in range(min(unroll, most - low)):
                code = code_ref[d, low + k]
                line = flat_ref[pl.ds(lax.shift_right_logical(code, LANES.bit_length() - 1), 1), :]
                found.append(jnp.where(lane == (code & (LANES - 1)), line, 0.0))
            for k, line in enumerate(found):
                lines_ref[pl.ds(base + (low + k), 1), :] = line
        return carry

    lax.fori_loop(0, devices, outer, 0)
    ones = jnp.ones((SUB, LANES), F32)
    found = dot(ones, lines_ref[...], ((1,), (1,)))
    out_ref[...] = jnp.zeros_like(out_ref)
    if extra_ref is not None:
        out_ref[:, most : most + 2] = jnp.broadcast_to(extra_ref[0:1, 0:2], (devices, 2))
    for d in range(devices):
        out_ref[d : d + 1, 0:most] = found[0:1, d * most : (d + 1) * most]


def gather_kernel(most, code_ref, field_ref, out_ref, lines_ref, flat_ref):
    across = field_ref.shape[1] // LANES

    def flatten(j, carry):
        for k in range(2):
            for t in range(across):
                to = pl.ds(pl.multiple_of(((2 * j + k) * across + t) * SUB, SUB), SUB)
                at = pl.ds(pl.multiple_of((2 * j + k) * SUB, SUB), SUB)
                flat_ref[to, :] = field_ref[at, t * LANES : (t + 1) * LANES]
        return carry

    lax.fori_loop(0, field_ref.shape[0] // (2 * SUB), flatten, 0)
    gather_cells(most, code_ref, flat_ref, None, out_ref, lines_ref)


def sweep_kernel(rows, most, first, opening, closing, sending, carrying, *refs):
    refs = list(refs)
    me_ref, field_ref, near_ref, far_ref, rhs_ref, scale_ref = refs[:6]
    del refs[:6]
    if opening or closing:
        code_ref = refs.pop(0)
    if opening:
        value_ref = refs.pop(0)
    extra_ref = refs.pop(0) if closing and carrying else None
    out_ref = refs.pop(0)
    sends = [refs.pop(0), refs.pop(0)] if sending else []
    grids = []
    if opening:
        source_ref, *grids = refs
        scatter_cells(most, first, code_ref, value_ref, grids)
    if closing:
        sampled_ref, lines_ref, flat_ref = refs
    wide, depth = near_ref.shape
    across = depth // LANES
    sub = iota((SUB, depth), 0)
    lane = iota((SUB, depth), 1)
    even = (me_ref[0] & 1) == 0
    blocks = wide // SUB
    unroll = 2

    def block(j):
        y = pl.multiple_of(j * SUB, SUB)
        above = pl.multiple_of(jnp.maximum(j - 1, 0) * SUB, SUB)
        below = pl.multiple_of(jnp.minimum(j + 1, blocks - 1) * SUB, SUB)
        top = (sub == 0) & (j == 0)
        bottom = (sub == SUB - 1) & (j == blocks - 1)
        near, far = near_ref[pl.ds(y, SUB), :], far_ref[pl.ds(y, SUB), :]
        low, high = jnp.where(even, far, near), jnp.where(even, near, far)
        tiles = [field_ref[pl.ds(x * wide + y, SUB), :] for x in range(rows)]
        edge = []
        for x, here in enumerate(tiles):
            spot = pl.ds(x * wide + y, SUB)
            over = field_ref[pl.ds(x * wide + above, SUB), :]
            under = field_ref[pl.ds(x * wide + below, SUB), :]
            beside = (low if x == 0 else tiles[x - 1]) + (high if x == rows - 1 else tiles[x + 1])
            ahead = pltpu.roll(jnp.where(sub == SUB - 1, over, here), 1, 0)
            behind = pltpu.roll(jnp.where(sub == 0, under, here), SUB - 1, 0)
            beside = beside + jnp.where(top, 0.0, ahead)
            beside = beside + jnp.where(bottom, 0.0, behind)
            beside = beside + jnp.where(lane == 0, 0.0, pltpu.roll(here, 1, 1))
            beside = beside + jnp.where(lane == depth - 1, 0.0, pltpu.roll(here, depth - 1, 1))
            rhs = rhs_ref[spot, :]
            at = (x * blocks + j) * across
            if grids:
                parts = []
                for t in range(across):
                    part = grids[0][at + t]
                    for grid in grids[1:]:
                        part = part + grid[at + t]
                    parts.append(part)
                rhs = rhs + jnp.concatenate(parts, axis=1)
                source_ref[spot, :] = rhs
            new = (1.0 - OMEGA) * here + (rhs + beside) * scale_ref[spot, :]
            out_ref[spot, :] = new
            if closing:
                for t in range(across):
                    to = pl.ds(pl.multiple_of((at + t) * SUB, SUB), SUB)
                    flat_ref[to, :] = new[:, t * LANES : (t + 1) * LANES]
            if x in (0, rows - 1):
                edge.append(new)
        if sending:
            sends[0][pl.ds(y, SUB), :] = jnp.where(even, edge[1], edge[0])
            sends[1][pl.ds(y, SUB), :] = jnp.where(even, edge[0], edge[1])

    def step(j, carry):
        for k in range(unroll):
            block(j * unroll + k)
        return carry

    lax.fori_loop(0, blocks // unroll, step, 0)
    if closing:
        gather_cells(most, code_ref, flat_ref, extra_ref, sampled_ref, lines_ref)


def stencil(field, stiff, layers, edge=None):
    sub = iota(field[0].shape, 0)
    turns = field[0].shape[1]
    out = []
    for index, here in enumerate(field):
        layer = index % layers
        before, after = pltpu.roll(here, 1, 0), pltpu.roll(here, SUB - 1, 0)
        if edge is not None:
            before = jnp.where(sub == 0, edge[index][0], before)
            after = jnp.where(sub == SUB - 1, edge[index][1], after)
        beside = before + after + pltpu.roll(here, 1, 1) + pltpu.roll(here, turns - 1, 1)
        if layer > 0:
            beside = beside + field[index - 1]
        if layer < layers - 1:
            beside = beside + field[index + 1]
        out.append((6.0 + stiff[layer]) * here - beside)
    return out


def inner(left, right, own):
    total = jnp.zeros_like(left[0])
    for a, b in zip(left, right):
        total = total + a * b
    return jnp.sum(jnp.where(own, total, 0.0), keepdims=True)


def wall_parts(force, stiff, layers, valid, own, force_ref, image_ref, twice_ref):
    force = [jnp.where(valid, tile, 0.0) for tile in force]
    image = [jnp.where(valid, tile, 0.0) for tile in stencil(force, stiff, layers)]
    twice = stencil(image, stiff, layers)
    for index in range(len(force)):
        force_ref[index] = force[index]
        image_ref[index] = image[index]
        twice_ref[index] = twice[index]
    return inner(force, force, own), inner(force, image, own)


def row_masks(me, devices, rows, shape):
    lead = (SUB - rows) // 2
    sub = iota(shape, 0)
    valid = ((sub >= lead) | (me > 0)) & ((sub < lead + rows) | (me < devices - 1))
    own = (sub >= lead) & (sub < lead + rows)
    return valid, own


def two_lanes(first, second, lanes):
    lane = iota((1, lanes), 1)
    return jnp.where(lane == 0, first, jnp.where(lane == 1, second, 0.0))


def pack_kernel(layers, rows, me_ref, start_ref, load_ref, stiff_ref, state_ref, near_ref, far_ref, own_ref):
    even = (me_ref[0] & 1) == 0
    turns = start_ref.shape[3]
    lead = (SUB - rows) // 2
    tiles = 3 * layers
    for c in range(3):
        for s in range(rows):
            own_ref[c, s : s + 1, :] = state_ref[3 + c : 4 + c, s * turns : (s + 1) * turns]
    at = 0
    near_ref[...] = jnp.zeros_like(near_ref)
    far_ref[...] = jnp.zeros_like(far_ref)
    for kind, count in enumerate((tiles, tiles, layers, 3)):
        deep = lead + 1 if kind == 0 else lead
        for i in range(count):
            if kind == 0:
                tile = start_ref[i // layers, i % layers]
            elif kind == 1:
                tile = load_ref[i // layers, i % layers]
            else:
                tile = stiff_ref[i] if kind == 2 else own_ref[i]
            first, last = tile[0:deep, :], tile[rows - deep : rows, :]
            near_ref[at : at + deep, :] = jnp.where(even, last, first)
            far_ref[at : at + deep, :] = jnp.where(even, first, last)
            at += deep


def wall_first_kernel(devices, layers, me_ref, start_ref, load_ref, stiff_in_ref, state_ref, near_ref, far_ref, past_ref,
                      send_ref, base_ref, stiff_ref, force_ref, image_ref, twice_ref, wide_ref):
    rows, turns = start_ref.shape[2:]
    lead = (SUB - rows) // 2
    tiles = 3 * layers
    even = (me_ref[0] & 1) == 0
    edge, at = [], 0
    for kind, count in enumerate((tiles, tiles, layers, 3)):
        deep = lead + 1 if kind == 0 else lead
        for i in range(count):
            near, far = near_ref[at : at + deep, :], far_ref[at : at + deep, :]
            low, high = jnp.where(even, far, near), jnp.where(even, near, far)
            to = (0, tiles, 2 * tiles, 2 * tiles + layers)[kind] + i
            wide_ref[to, 0:lead, :] = low[deep - lead : deep, :]
            wide_ref[to, lead + rows : SUB, :] = high[0:lead, :]
            if kind == 0:
                edge.append((low[0:1, :], high[lead:deep, :]))
                wide_ref[to, lead : lead + rows, :] = start_ref[i // layers, i % layers]
            elif kind == 1:
                wide_ref[to, lead : lead + rows, :] = load_ref[i // layers, i % layers]
            elif kind == 2:
                wide_ref[to, lead : lead + rows, :] = stiff_in_ref[i]
            else:
                for s in range(rows):
                    wide_ref[to, lead + s : lead + s + 1, :] = state_ref[3 + i : 4 + i, s * turns : (s + 1) * turns]
            at += deep
    start = [wide_ref[i] for i in range(tiles)]
    stiff = [wide_ref[2 * tiles + i] for i in range(layers)]
    for i in range(layers):
        stiff_ref[i] = stiff[i]
    applied = stencil(start, stiff, layers, edge)
    for i in range(tiles):
        base_ref[i] = wide_ref[tiles + i] - applied[i]
    valid, own = row_masks(me_ref[0], devices, rows, (SUB, turns))
    force = [base_ref[i] for i in range(tiles)]
    for c in range(3):
        force[c * layers] = force[c * layers] + wide_ref[2 * tiles + layers + c]
    square, product = wall_parts(force, stiff, layers, valid, own, force_ref, image_ref, twice_ref)
    history = past_ref.shape[1]
    gram = jnp.zeros((history, history), F32)
    for c in range(past_ref.shape[0]):
        gram = gram + dot(past_ref[c], past_ref[c], ((1,), (1,)))
    send_ref[...] = jnp.broadcast_to(two_lanes(square, product, LANES), (devices, LANES))
    chunk = history * history // devices
    for d in range(devices):
        row, left = d * chunk // history, d * chunk % history
        send_ref[d : d + 1, 2 : 2 + chunk] = gram[row : row + 1, left : left + chunk]


def wall_next_kernel(devices, layers, rows, me_ref, near_ref, far_ref, state_ref, base_ref, stiff_ref,
                     send_ref, force_ref, image_ref, twice_ref, pull_ref):
    tiles, _, turns = base_ref.shape
    lead = (SUB - rows) // 2
    me = me_ref[0]
    even = (me & 1) == 0
    for c in range(3):
        near, far = near_ref[c : c + 1, :], far_ref[c : c + 1, :]
        low, high = jnp.where(even, far, near), jnp.where(even, near, far)
        for s in range(rows):
            pull_ref[c, lead + s : lead + s + 1, :] = state_ref[3 + c : 4 + c, s * turns : (s + 1) * turns]
        for s in range(lead):
            pull_ref[c, s : s + 1, :] = low[:, s * turns : (s + 1) * turns]
            pull_ref[c, lead + rows + s : lead + rows + s + 1, :] = high[:, s * turns : (s + 1) * turns]
    valid, own = row_masks(me, devices, rows, (SUB, turns))
    force = [base_ref[i] for i in range(tiles)]
    for c in range(3):
        force[c * layers] = force[c * layers] + pull_ref[c]
    stiff = [stiff_ref[i] for i in range(layers)]
    square, product = wall_parts(force, stiff, layers, valid, own, force_ref, image_ref, twice_ref)
    send_ref[...] = jnp.broadcast_to(two_lanes(square, product, LANES), (devices, LANES))


def summed(got_ref):
    return jnp.sum(got_ref[...], axis=0, keepdims=True)


def wall_second_kernel(rows, got_ref, force_ref, image_ref, twice_ref, send_ref):
    total = summed(got_ref)
    alpha = total[:, 0:1] / total[:, 1:2]
    shape = force_ref.shape[1:]
    lead = (SUB - rows) // 2
    sub = iota(shape, 0)
    own = (sub >= lead) & (sub < lead + rows)
    square = jnp.zeros(shape, F32)
    product = jnp.zeros(shape, F32)
    for i in range(force_ref.shape[0]):
        residual = force_ref[i] - alpha * image_ref[i]
        image = image_ref[i] - alpha * twice_ref[i]
        square = square + residual * residual
        product = product + residual * image
    square = jnp.sum(jnp.where(own, square, 0.0), keepdims=True)
    product = jnp.sum(jnp.where(own, product, 0.0), keepdims=True)
    lane = iota((1, LANES), 1)
    row = jnp.where(lane == 0, square, jnp.where(lane == 1, product, total))
    send_ref[...] = jnp.broadcast_to(row, send_ref.shape)


def wall_last_kernel(layers, rows, at, one_ref, two_ref, force_ref, image_ref, start_ref, wall_ref, solid_ref):
    one = summed(one_ref)
    two = jnp.sum(two_ref[:, at : at + 2], axis=0, keepdims=True)
    norm, alpha = one[:, 0:1], one[:, 0:1] / one[:, 1:2]
    newer = two[:, 0:1]
    ratio = newer / norm
    beta = newer / (two[:, 1:2] - ratio * newer / alpha)
    turns = force_ref.shape[2]
    lead = (SUB - rows) // 2
    for i in range(force_ref.shape[0]):
        c, layer = i // layers, i % layers
        force = force_ref[i]
        residual = force - alpha * image_ref[i]
        moved = alpha * force + beta * (residual + ratio * force)
        wall = start_ref[c, layer] + moved[lead : lead + rows, :]
        wall_ref[c, layer] = wall
        if layer == 0:
            for s in range(rows):
                solid_ref[c : c + 1, s * turns : (s + 1) * turns] = wall[s : s + 1, :]


def returned_kernel(devices, most, turn, got_ref, owner_ref, rank_ref, normals_ref, state_ref, solid_ref, past_ref, *rest):
    if turn == 0:
        output_ref, resid_ref, send_ref = rest
    else:
        last_ref, output_ref, resid_ref, send_ref = rest
    named, placed = onehots(owner_ref[...], rank_ref[...], devices, most)
    spread = dot(got_ref[:, 0:most], named, ((0,), (0,)))
    sampled = jnp.sum(spread * placed, axis=0, keepdims=True)
    output_ref[0:3, :] = solid_ref[...]
    output_ref[3:6, :] = -sampled * normals_ref[...]
    resid_ref[...] = output_ref[...] - state_ref[...]
    history = past_ref.shape[1]
    points = state_ref.shape[1]
    sub = iota((SUB, points), 0)
    parts = jnp.zeros((SUB, history), F32)
    newest = jnp.zeros((SUB, SUB), F32)
    for c in range(6):
        resid = resid_ref[c : c + 1, :]
        pair = jnp.where(sub == 0, resid, 0.0)
        if turn > 0:
            pair = jnp.where(sub == 1, resid - last_ref[c : c + 1, :], pair)
            newest = newest + dot(pair, pair, ((1,), (1,)))
        parts = parts + dot(pair, past_ref[c], ((1,), (1,)))
    send_ref[...] = jnp.zeros_like(send_ref)
    send_ref[:, 0:history] = jnp.broadcast_to(parts[0:1, :], (devices, history))
    if turn > 0:
        send_ref[:, history : 2 * history] = jnp.broadcast_to(parts[1:2, :], (devices, history))
        send_ref[:, 2 * history : 2 * history + 2] = jnp.broadcast_to(newest[1:2, 0:2], (devices, 2))


def gram_of(gram_ref, history, work_ref):
    devices = gram_ref.shape[0]
    chunk = history * history // devices
    for d in range(devices):
        row, left = d * chunk // history, d * chunk % history
        work_ref[row : row + 1, left : left + chunk] = gram_ref[d : d + 1, 2 : 2 + chunk]


def eliminated(table, history):
    sub, lane = iota(table.shape, 0), iota(table.shape, 1)
    diagonal = (sub == lane) & (sub < history)
    trace = jnp.sum(jnp.where(diagonal, table, 0.0), keepdims=True)
    ridge = RIDGE * trace / history + TINY
    table = jnp.where(diagonal, table + ridge, table)
    table = jnp.where((lane == sub + history) & (sub < history), 1.0, table)
    for k in range(0, history, 2):
        first, second = table[k : k + 1, :], table[k + 1 : k + 2, :]
        top, cross, low = first[:, k : k + 1], first[:, k + 1 : k + 2], second[:, k + 1 : k + 2]
        scale = 1.0 / (top * low - cross * cross)
        left = jnp.where(sub[:, 0:1] > k + 1, table[:, k : k + 1], 0.0)
        right = jnp.where(sub[:, 0:1] > k + 1, table[:, k + 1 : k + 2], 0.0)
        table = table - left * ((low * first - cross * second) * scale) - right * ((top * second - cross * first) * scale)
    return table[history:, history : 2 * history]


def inverse_kernel(history, gram_ref, out_ref, work_ref):
    work_ref[...] = jnp.zeros_like(work_ref)
    gram_of(gram_ref, history, work_ref)
    sub, lane = iota(work_ref.shape, 0), iota(work_ref.shape, 1)
    table = jnp.where((sub == lane + history) & (lane < history), 1.0, work_ref[...])
    out_ref[...] = eliminated(table, history)


def coefficients(history, got_ref, gram_ref, work_ref):
    total = summed(got_ref)
    work_ref[...] = jnp.zeros_like(work_ref)
    gram_of(gram_ref, history, work_ref)
    sub, lane = iota(work_ref.shape, 0), iota(work_ref.shape, 1)
    swap = history - 1
    fresh = total[:, history : 2 * history]
    square = total[:, 2 * history + 1 : 2 * history + 2]
    along = total[:, 2 * history : 2 * history + 1]
    edge = iota((1, history), 1) == swap
    work_ref[swap : swap + 1, 0:history] = jnp.where(edge, square, fresh)
    work_ref[history : history + 1, 0:history] = jnp.where(edge, along, total[:, 0:history])
    line = work_ref[swap : swap + 1, :]
    column = jnp.sum(jnp.where(sub == lane, line, 0.0), axis=1, keepdims=True)
    table = jnp.where((lane == swap) & (sub < history), column, work_ref[...])
    return eliminated(table, history)[0:1]


def update_kernel(devices, most, lead, turns, me_ref, got_ref, inverse_ref, output_ref, past_ref, owner_ref, rank_ref, normals_ref,
                  next_ref, send_ref, near_ref, far_ref):
    history = past_ref.shape[1]
    total = summed(got_ref)
    rows = dot(jnp.broadcast_to(total[:, 0:history], (SUB, history)), inverse_ref[...], ((1,), (0,)))
    for c in range(6):
        next_ref[c : c + 1, :] = output_ref[c : c + 1, :] + dot(rows, past_ref[c], ((1,), (0,)))[0:1, :]
    me = me_ref[0]
    points = output_ref.shape[1]
    named, placed = onehots(owner_ref[...], rank_ref[...], devices, most)
    flux = flux_of(normals_ref[...], next_ref[...])
    send_ref[...] = jnp.zeros_like(send_ref)
    send_ref[:, 0:most] = dot(named, placed * flux, ((1,), (1,)))
    half = lead * turns
    even = (me & 1) == 0
    for c in range(3):
        first, last = next_ref[3 + c : 4 + c, 0:half], next_ref[3 + c : 4 + c, points - half : points]
        near_ref[c : c + 1, :] = jnp.where(even, last, first)
        far_ref[c : c + 1, :] = jnp.where(even, first, last)


def finish_kernel(got_ref, gram_ref, output_ref, past_ref, last_ref, next_ref, work_ref):
    history = past_ref.shape[1]
    coeffs = coefficients(history, got_ref, gram_ref, work_ref)
    swap = history - 1
    newest = coeffs[:, swap:history]
    rows = jnp.broadcast_to(coeffs, (SUB, history))
    rows = jnp.where(iota(rows.shape, 1) == swap, 0.0, rows)
    for c in range(6):
        here = output_ref[c : c + 1, :]
        moved = dot(rows, past_ref[c], ((1,), (0,)))[0:1, :]
        next_ref[c : c + 1, :] = here + moved + newest * (here - last_ref[c : c + 1, :])


def local(
    pressure_start,
    fluid_coef,
    fluid_rhs,
    wall_start,
    wall_stiff,
    wall_load,
    normals,
    fluid_owner,
    fluid_cell,
    interface_start,
    past_residual,
    past_output,
):
    devices = lax.axis_size(AXES)
    me = lax.axis_index(AXES).astype(jnp.int32).reshape(1)
    rows, wide, depth = pressure_start.shape
    points = fluid_cell.shape[0]
    most = max(2, 2 * points // devices)
    history = past_residual.shape[0]
    layers, wall_rows, turns = wall_stiff.shape
    flat = (rows * wide, depth)
    plane = (wide, depth)
    lead = (SUB - wall_rows) // 2
    tiles = 3 * layers
    tile = (tiles, SUB, turns)
    slots = LANES * -(-2 * most // LANES)

    owner = fluid_owner.reshape(1, points)
    field = pressure_start.reshape(flat)
    low, high = field[0:wide], field[flat[0] - wide :]
    even = (me[0] & 1) == 0
    ends = tie(jnp.where(even, high, low), jnp.where(even, low, high))
    near, far = swap(*ends)
    past_r = jnp.transpose(past_residual, (1, 0, 2))
    past_w = jnp.transpose(past_output, (1, 0, 2))
    rhs = fluid_rhs.reshape(flat)

    owner, _ = tie(owner, ends)
    send, rank = call(
        functools.partial(route_kernel, devices, most),
        [((devices, slots), F32), ((1, points), jnp.int32)],
        [vmem()] * 4, limit=4,
    )(owner, fluid_cell.reshape(1, points), normals, interface_start)
    got = exchange(send)
    got, coef, start_in, load_in, state = tie(got, fluid_coef, wall_start, wall_load, interface_start)
    cells = tiled_place(jnp.maximum(got[:, 0:most].astype(jnp.int32) - 1, 0), depth)
    flux, spot = got, most
    scale = (OMEGA / (6.0 + coef)).reshape(flat)

    needed = (3 * (lead + 1) + 3 * lead + lead) * layers + 3 * lead
    packed = (SUB * -(-needed // SUB), turns)
    packs = call(
        functools.partial(pack_kernel, layers, wall_rows),
        [(packed, F32)] * 2, [smem()] + [vmem()] * 4, [pltpu.VMEM((3, wall_rows, turns), F32)], limit=2,
    )(me, start_in, load_in, wall_stiff, state)

    small = ((devices, LANES), F32)
    padded = LANES * -(-2 * history // LANES)
    output = resid = wall = None
    for turn in range(COUPLE):
        for sweep in range(SWEEPS):
            last = sweep + 1 == SWEEPS
            sending = not last or turn + 1 < COUPLE
            opening, closing = sweep == 0, not sending
            carrying = turn > 0
            extra_in, extra_spec, extra_out, scratch = [], [], [], []
            if opening:
                extra_in, extra_spec = [cells, flux], [smem(), smem()]
                extra_out = [(flat, F32)]
                scratch = [pltpu.VMEM((flat[0] * depth // (SUB * LANES), SUB, LANES), F32)] * GRIDS
            if closing:
                extra_in, extra_spec = [cells], [smem()]
                if carrying:
                    sums = call(
                        functools.partial(wall_second_kernel, wall_rows),
                        [((SUB, LANES), F32)], [vmem()] * 4, limit=2,
                    )(one, force, image, twice)[0]
                    extra_in, extra_spec = [cells, sums], [smem(), vmem()]
                extra_out = [((devices, LANES * -(-(most + 2) // LANES)), F32)]
                scratch = [pltpu.VMEM((devices * most, LANES), F32), pltpu.VMEM((flat[0] * depth // LANES, LANES), F32)]
            field, *rest = call(
                functools.partial(sweep_kernel, rows, most, spot, opening, closing, sending, carrying),
                [(flat, F32)] + [(plane, F32)] * (2 if sending else 0) + extra_out,
                [smem()] + [vmem()] * 5 + extra_spec, scratch, limit=26 if opening else 12,
            )(me, field, near, far, rhs if opening else source, scale, *extra_in)
            if sending:
                ends, rest = rest[:2], rest[2:]
            if opening:
                source = rest[0]
            if closing:
                sampled = rest[0]
            elif last:
                near, far = swap(*ends)
                sampled = call(
                    functools.partial(gather_kernel, most),
                    [((devices, LANES * -(-most // LANES)), F32)],
                    [smem(), vmem()],
                    [pltpu.VMEM((devices * most, LANES), F32), pltpu.VMEM((flat[0] * depth // LANES, LANES), F32)],
                    limit=12,
                )(cells, field)[0]
            else:
                near, far = swap(*ends)
            if turn == 0 and sweep == 0:
                packs, _ = tie(packs, ends)
                pack_near, pack_far = swap(*packs)
                far, pack_far = tie(far, pack_far)
            if turn == 0 and sweep == 1:
                pack_near, ends = tie(pack_near, ends)
                sums, base, stiff, force, image, twice = call(
                    functools.partial(wall_first_kernel, devices, layers),
                    [small, (tile, F32), ((layers, SUB, turns), F32)] + [(tile, F32)] * 3,
                    [smem()] + [vmem()] * 7,
                    [pltpu.VMEM((2 * tiles + layers + 3, SUB, turns), F32)], limit=6,
                )(me, start_in, load_in, wall_stiff, state, pack_near, pack_far, past_r)
                one = exchange(sums)
                one, far = tie(one, far)
            if turn == 0 and sweep == 2:
                one, ends = tie(one, ends)
                sums = call(
                    functools.partial(wall_second_kernel, wall_rows),
                    [small], [vmem()] * 4, limit=2,
                )(one, force, image, twice)[0]
                two = exchange(sums)
                inverse = call(
                    functools.partial(inverse_kernel, history),
                    [((history, history), F32)], [vmem()], [pltpu.VMEM((2 * history, padded), F32)], limit=2,
                )(two)[0]
                wall, solid = call(
                    functools.partial(wall_last_kernel, layers, wall_rows, 0),
                    [(wall_start.shape, F32), ((3, points), F32)], [vmem()] * 5, limit=2,
                )(one, two, force, image, wall_start)
                inverse, far, solid = tie(inverse, far, solid)
                grams = two
            if turn == 1 and sweep == 0:
                pulls, ends = tie(pulls, ends)
                pull_near, pull_far = swap(*pulls)
                far, pull_far = tie(far, pull_far)
            if turn == 1 and sweep == 1:
                pull_near, ends = tie(pull_near, ends)
                sums, force, image, twice = call(
                    functools.partial(wall_next_kernel, devices, layers, wall_rows),
                    [small, (tile, F32), (tile, F32), (tile, F32)],
                    [smem()] + [vmem()] * 5,
                    [pltpu.VMEM((3, SUB, turns), F32)], limit=2,
                )(me, pull_near, pull_far, state, base, stiff)
                one = exchange(sums)
                one, far = tie(one, far)
        back = exchange(sampled)
        if turn + 1 == COUPLE:
            wall, solid = call(
                functools.partial(wall_last_kernel, layers, wall_rows, most),
                [(wall_start.shape, F32), ((3, points), F32)], [vmem()] * 5, limit=2,
            )(one, back, force, image, wall_start)
        last_args = () if turn == 0 else (resid,)
        before = output
        output, resid, sums = call(
            functools.partial(returned_kernel, devices, most, turn),
            [((6, points), F32), ((6, points), F32), ((devices, LANES * -(-(2 * history + 2) // LANES)), F32)],
            [vmem()] * (7 + len(last_args)), limit=4,
        )(back, owner, rank, normals, state, solid, past_r, *last_args)
        if turn + 1 < COUPLE:
            sums, inverse = tie(sums, inverse)
        total = exchange(sums)
        if turn + 1 < COUPLE:
            state, flux, *pulls = call(
                functools.partial(update_kernel, devices, most, lead, turns),
                [((6, points), F32), ((devices, LANES * -(-most // LANES)), F32)] + [((3, lead * turns), F32)] * 2,
                [smem()] + [vmem()] * 7, limit=4,
            )(me, total, inverse, output, past_w, owner, rank, normals)
            flux, spot = exchange(flux), 0
            flux, pulls = tie(flux, pulls)
        else:
            work = [pltpu.VMEM((SUB * -(-(history + 1) // SUB), padded), F32)]
            state = call(
                finish_kernel, [((6, points), F32)], [vmem()] * 5, work, limit=4,
            )(total, grams, output, past_w, before)[0]
    return (state, field.reshape(pressure_start.shape), wall)


def solution(mesh):
    placed = (
        P(("solver", "space"), None, None),
        P(("solver", "space"), None, None),
        P(("solver", "space"), None, None),
        P(None, None, ("solver", "space"), None),
        P(None, ("solver", "space"), None),
        P(None, None, ("solver", "space"), None),
        P(None, ("solver", "space")),
        P(("solver", "space"), None),
        P(("solver", "space")),
        P(None, ("solver", "space")),
        P(None, None, ("solver", "space")),
        P(None, None, ("solver", "space")),
    )

    return jax.shard_map(
        local,
        mesh=mesh,
        in_specs=placed,
        out_specs=(
            P(None, ("solver", "space")),
            P(("solver", "space"), None, None),
            P(None, None, ("solver", "space"), None),
        ),
        check_vma=False,
    )
```

```python
import functools

import jax
import jax.numpy as jnp
from jax import lax
from jax.experimental import pallas as pl
from jax.experimental.pallas import tpu as pltpu
from jax.sharding import PartitionSpec as P


SWEEPS = 4
COUPLE = 2

OMEGA = 0.8
SOURCE_GAIN = 4.0
RIDGE = 0.1
TINY = 1e-06

AXES = ("solver", "space")
LANES = 128
GRIDS = 4
SUB = 8
HIGHEST = lax.Precision.HIGHEST
F32 = jnp.float32


def vmem():
    return pl.BlockSpec(memory_space=pltpu.VMEM)


def smem():
    return pl.BlockSpec(memory_space=pltpu.SMEM)


def call(kernel, outs, ins, scratch=(), limit=16):
    return pl.pallas_call(
        kernel,
        out_shape=[jax.ShapeDtypeStruct(shape, dtype) for shape, dtype in outs],
        in_specs=ins,
        out_specs=[vmem() for _ in outs],
        scratch_shapes=list(scratch),
        compiler_params=pltpu.CompilerParams(vmem_limit_bytes=limit * 1024 * 1024),
    )


def dot(a, b, dims):
    return lax.dot_general(a, b, (dims, ((), ())), precision=HIGHEST, preferred_element_type=F32)


def iota(shape, dim):
    return lax.broadcasted_iota(jnp.int32, shape, dim)


def exchange(send):
    return lax.all_to_all(send, AXES, split_axis=0, concat_axis=0, tiled=True)


def tie(*values):
    return lax.optimization_barrier(values)


def pairs():
    count = lax.axis_size(AXES)
    near = [(i, i ^ 1) for i in range(count)]
    up = [(i, i + 1) for i in range(1, count - 1, 2)]
    return near, up + [(target, source) for source, target in up]


def swap(near, far):
    first, second = pairs()
    far = lax.ppermute(far, AXES, second)
    return lax.ppermute(near, AXES, first), far


def onehots(owner, rank, devices, most):
    points = owner.shape[1]
    named = (owner == iota((devices, points), 0)).astype(F32)
    placed = (rank == iota((most, points), 0)).astype(F32)
    return named, placed


def flux_of(normals, state):
    product = normals * state[0:3]
    return SOURCE_GAIN * (product[0:1] + product[1:2] + product[2:3])


def route_kernel(devices, most, owner_ref, cell_ref, normals_ref, state_ref, send_ref, rank_ref):
    points = owner_ref.shape[1]
    owner = owner_ref[...]
    named = (owner == iota((devices, points), 0)).astype(F32)
    blocks = [named[:, i * LANES : (i + 1) * LANES] for i in range(points // LANES)]
    earlier = (iota((LANES, LANES), 0) < iota((LANES, LANES), 1)).astype(jnp.bfloat16)
    base = jnp.zeros((devices, 1), F32)
    for i, block in enumerate(blocks):
        ahead = jnp.dot(block.astype(jnp.bfloat16), earlier, preferred_element_type=F32) + base
        rank_ref[:, i * LANES : (i + 1) * LANES] = jnp.sum(ahead * block, axis=0, keepdims=True).astype(jnp.int32)
        base = base + jnp.sum(block, axis=1, keepdims=True)
    placed = (rank_ref[...] == iota((most, points), 0)).astype(F32)
    flux = flux_of(normals_ref[...], state_ref[...])
    marks = (cell_ref[...] + 1).astype(F32)
    send_ref[...] = jnp.zeros_like(send_ref)
    send_ref[:, 0:most] = dot(named, placed * marks, ((1,), (1,)))
    send_ref[:, most : 2 * most] = dot(named, placed * flux, ((1,), (1,)))


def places(cell, rows, depth):
    row, along = cell // depth, cell % depth
    line = (along // LANES) * rows + row
    lane = along % LANES
    inside = (line % SUB) * LANES + lane
    return (line - line % SUB) * (SUB * LANES) + inside, line * LANES + lane


def scatter_cells(most, first, code_ref, value_ref, grids):
    count = len(grids)
    place = iota((SUB, LANES), 0) * LANES + iota((SUB, LANES), 1)
    area = SUB * LANES
    fill = 64

    def clear(step, carry):
        for grid in grids:
            grid[pl.ds(pl.multiple_of(step * fill, fill), fill), :] = jnp.zeros((fill, LANES), F32)
        return carry

    lax.fori_loop(0, grids[0].shape[0] // fill, clear, 0)
    part = code_ref.shape[0] // count

    def outer(d, carry):
        for slot in range(most):
            codes = [code_ref[g * part + d, slot] for g in range(count)]
            tiles = [pl.multiple_of(lax.shift_right_logical(code, area.bit_length() - 1), SUB) for code in codes]
            tiles = [(pl.ds(tile, SUB), slice(None)) for tile in tiles]
            added = [
                grid[tile] + jnp.where(place == (code & (area - 1)), value_ref[g * part + d, first + slot], 0.0)
                for g, (grid, tile, code) in enumerate(zip(grids, tiles, codes))
            ]
            for grid, tile, new in zip(grids, tiles, added):
                grid[tile] = new
        return carry

    lax.fori_loop(0, part, outer, 0)


def gather_cells(most, code_ref, flat_ref, extra_ref, out_ref, lines_ref):
    devices = code_ref.shape[0]
    lane = iota((1, LANES), 1)
    unroll = 16

    def outer(d, carry):
        base = pl.multiple_of(d * most, SUB)
        for low in range(0, most, unroll):
            found = []
            for k in range(min(unroll, most - low)):
                code = code_ref[d, low + k]
                line = flat_ref[pl.ds(lax.shift_right_logical(code, LANES.bit_length() - 1), 1), :]
                found.append(jnp.where(lane == (code & (LANES - 1)), line, 0.0))
            for k, line in enumerate(found):
                lines_ref[pl.ds(base + (low + k), 1), :] = line
        return carry

    lax.fori_loop(0, devices, outer, 0)
    ones = jnp.ones((SUB, LANES), F32)
    found = dot(ones, lines_ref[...], ((1,), (1,)))
    out_ref[...] = jnp.zeros_like(out_ref)
    if extra_ref is not None:
        out_ref[:, most : most + 2] = jnp.broadcast_to(extra_ref[0:1, 0:2], (devices, 2))
    for d in range(devices):
        out_ref[d : d + 1, 0:most] = found[0:1, d * most : (d + 1) * most]


def gather_kernel(most, code_ref, field_ref, extra_ref, out_ref, lines_ref):
    gather_cells(most, code_ref, field_ref, extra_ref, out_ref, lines_ref)


def sweep_kernel(rows, most, first, opening, closing, sending, carrying, fetching, *refs):
    refs = list(refs)
    me_ref, field_ref, near_ref, far_ref, rhs_ref, scale_ref = refs[:6]
    del refs[:6]
    if opening or closing:
        code_ref = refs.pop(0)
    if opening:
        value_ref = refs.pop(0)
    extra_ref = refs.pop(0) if closing and carrying else None
    out_ref = refs.pop(0)
    sends = [refs.pop(0), refs.pop(0)] if sending else []
    grids = []
    if opening:
        source_ref, *grids = refs
        copies = []
        scaled_ref = grids.pop(0) if fetching else None
        if fetching:
            *grids, field_in, rhs_in, scale_in, sems = grids
            moves = ((field_ref, field_in), (rhs_ref, rhs_in), (scale_ref, scale_in))
            copies = [pltpu.make_async_copy(source, into, sems.at[i]) for i, (source, into) in enumerate(moves)]
            field_ref, rhs_ref, scale_ref = field_in, rhs_in, scale_in
        for copy in copies:
            copy.start()
        scatter_cells(most, first, code_ref, value_ref, grids)
        for copy in copies:
            copy.wait()
    if closing:
        sampled_ref, lines_ref, flat_ref = refs
    wide, depth = near_ref.shape
    across = depth // LANES
    sub = iota((SUB, LANES), 0)
    lane = iota((SUB, LANES), 1)
    even = (me_ref[0] & 1) == 0
    blocks = wide // SUB
    unroll = 2

    zero = jnp.zeros((SUB, LANES), F32)
    total = rows * wide
    strips = field_ref.shape[1] == LANES

    def block(j, first_block=False, last_block=False):
        y = pl.multiple_of(j * SUB, SUB)

        def tile(start, t):
            if strips:
                return field_ref[pl.ds(start + t * total, SUB), :]
            return field_ref[pl.ds(start, SUB), t * LANES : (t + 1) * LANES]

        for t in range(across):
            strip = slice(t * LANES, (t + 1) * LANES)
            near, far = near_ref[pl.ds(y, SUB), strip], far_ref[pl.ds(y, SUB), strip]
            low, high = jnp.where(even, far, near), jnp.where(even, near, far)
            edge = []
            for x in range(rows):
                start = pl.multiple_of(x * wide + y, SUB)
                spot = pl.ds(start, SUB)
                here = tile(start, t)
                beside = low if x == 0 else tile(start - wide, t)
                beside = beside + (high if x == rows - 1 else tile(start + wide, t))
                if strips and not first_block:
                    beside = beside + tile(start - 1, t)
                else:
                    over = zero if first_block else tile(start - SUB, t)
                    beside = beside + pltpu.roll(jnp.where(sub == SUB - 1, over, here), 1, 0)
                if strips and not last_block:
                    beside = beside + tile(start + 1, t)
                else:
                    under = zero if last_block else tile(start + SUB, t)
                    beside = beside + pltpu.roll(jnp.where(sub == 0, under, here), SUB - 1, 0)
                left = tile(start, t - 1) if t > 0 else zero
                right = tile(start, t + 1) if t < across - 1 else zero
                beside = beside + pltpu.roll(jnp.where(lane == LANES - 1, left, here), 1, 1)
                beside = beside + pltpu.roll(jnp.where(lane == 0, right, here), LANES - 1, 1)
                rhs = rhs_ref[spot, strip]
                lines = pl.ds(pl.multiple_of(start + t * total, SUB), SUB)
                if grids:
                    for grid in grids:
                        rhs = rhs + grid[lines, :]
                    source_ref[spot, strip] = rhs
                scale = scale_ref[spot, strip]
                if fetching:
                    scale = OMEGA / (6.0 + scale)
                    scaled_ref[spot, strip] = scale
                new = (1.0 - OMEGA) * here + (rhs + beside) * scale
                if closing:
                    out_ref[spot, strip] = new
                    flat_ref[lines, :] = new
                else:
                    out_ref[lines, :] = new
                if x in (0, rows - 1):
                    edge.append(new)
            if sending:
                sends[0][pl.ds(y, SUB), strip] = jnp.where(even, edge[1], edge[0])
                sends[1][pl.ds(y, SUB), strip] = jnp.where(even, edge[0], edge[1])

    def step(j, carry):
        for k in range(unroll):
            block(1 + j * unroll + k)
        return carry

    block(0, first_block=True)
    lax.fori_loop(0, (blocks - 2) // unroll, step, 0)
    for j in range(1 + (blocks - 2) // unroll * unroll, blocks - 1):
        block(j)
    block(blocks - 1, last_block=True)
    if closing:
        gather_cells(most, code_ref, flat_ref, extra_ref, sampled_ref, lines_ref)


def stencil(field, stiff, layers, edge=None):
    sub = iota(field[0].shape, 0)
    turns = field[0].shape[1]
    out = []
    for index, here in enumerate(field):
        layer = index % layers
        before, after = pltpu.roll(here, 1, 0), pltpu.roll(here, SUB - 1, 0)
        if edge is not None:
            before = jnp.where(sub == 0, edge[index][0], before)
            after = jnp.where(sub == SUB - 1, edge[index][1], after)
        beside = before + after + pltpu.roll(here, 1, 1) + pltpu.roll(here, turns - 1, 1)
        if layer > 0:
            beside = beside + field[index - 1]
        if layer < layers - 1:
            beside = beside + field[index + 1]
        out.append((6.0 + stiff[layer]) * here - beside)
    return out


def inner(left, right, own):
    total = jnp.zeros_like(left[0])
    for a, b in zip(left, right):
        total = total + a * b
    return jnp.sum(jnp.where(own, total, 0.0), keepdims=True)


def wall_parts(force, stiff, layers, valid, own, force_ref, image_ref, twice_ref):
    force = [jnp.where(valid, tile, 0.0) for tile in force]
    image = [jnp.where(valid, tile, 0.0) for tile in stencil(force, stiff, layers)]
    twice = stencil(image, stiff, layers)
    for index in range(len(force)):
        force_ref[index] = force[index]
        image_ref[index] = image[index]
        twice_ref[index] = twice[index]
    return inner(force, force, own), inner(force, image, own)


def row_masks(me, devices, rows, shape):
    lead = (SUB - rows) // 2
    sub = iota(shape, 0)
    valid = ((sub >= lead) | (me > 0)) & ((sub < lead + rows) | (me < devices - 1))
    own = (sub >= lead) & (sub < lead + rows)
    return valid, own


def two_lanes(first, second, lanes):
    lane = iota((1, lanes), 1)
    return jnp.where(lane == 0, first, jnp.where(lane == 1, second, 0.0))


def pack_kernel(layers, rows, me_ref, start_ref, load_ref, stiff_ref, state_ref, near_ref, far_ref, own_ref):
    even = (me_ref[0] & 1) == 0
    turns = start_ref.shape[3]
    lead = (SUB - rows) // 2
    tiles = 3 * layers
    for c in range(3):
        for s in range(rows):
            own_ref[c, s : s + 1, :] = state_ref[3 + c : 4 + c, s * turns : (s + 1) * turns]
    at = 0
    near_ref[...] = jnp.zeros_like(near_ref)
    far_ref[...] = jnp.zeros_like(far_ref)
    for kind, count in enumerate((tiles, tiles, layers, 3)):
        deep = lead + 1 if kind == 0 else lead
        for i in range(count):
            if kind == 0:
                tile = start_ref[i // layers, i % layers]
            elif kind == 1:
                tile = load_ref[i // layers, i % layers]
            else:
                tile = stiff_ref[i] if kind == 2 else own_ref[i]
            first, last = tile[0:deep, :], tile[rows - deep : rows, :]
            near_ref[at : at + deep, :] = jnp.where(even, last, first)
            far_ref[at : at + deep, :] = jnp.where(even, first, last)
            at += deep


def wall_first_kernel(devices, layers, me_ref, start_ref, load_ref, stiff_in_ref, state_ref, near_ref, far_ref, gram_ref,
                      send_ref, base_ref, stiff_ref, force_ref, image_ref, twice_ref, wide_ref):
    rows, turns = start_ref.shape[2:]
    lead = (SUB - rows) // 2
    tiles = 3 * layers
    even = (me_ref[0] & 1) == 0
    edge, at = [], 0
    for kind, count in enumerate((tiles, tiles, layers, 3)):
        deep = lead + 1 if kind == 0 else lead
        for i in range(count):
            near, far = near_ref[at : at + deep, :], far_ref[at : at + deep, :]
            low, high = jnp.where(even, far, near), jnp.where(even, near, far)
            to = (0, tiles, 2 * tiles, 2 * tiles + layers)[kind] + i
            wide_ref[to, 0:lead, :] = low[deep - lead : deep, :]
            wide_ref[to, lead + rows : SUB, :] = high[0:lead, :]
            if kind == 0:
                edge.append((low[0:1, :], high[lead:deep, :]))
                wide_ref[to, lead : lead + rows, :] = start_ref[i // layers, i % layers]
            elif kind == 1:
                wide_ref[to, lead : lead + rows, :] = load_ref[i // layers, i % layers]
            elif kind == 2:
                wide_ref[to, lead : lead + rows, :] = stiff_in_ref[i]
            else:
                for s in range(rows):
                    wide_ref[to, lead + s : lead + s + 1, :] = state_ref[3 + i : 4 + i, s * turns : (s + 1) * turns]
            at += deep
    start = [wide_ref[i] for i in range(tiles)]
    stiff = [wide_ref[2 * tiles + i] for i in range(layers)]
    for i in range(layers):
        stiff_ref[i] = stiff[i]
    applied = stencil(start, stiff, layers, edge)
    for i in range(tiles):
        base_ref[i] = wide_ref[tiles + i] - applied[i]
    valid, own = row_masks(me_ref[0], devices, rows, (SUB, turns))
    force = [base_ref[i] for i in range(tiles)]
    for c in range(3):
        force[c * layers] = force[c * layers] + wide_ref[2 * tiles + layers + c]
    square, product = wall_parts(force, stiff, layers, valid, own, force_ref, image_ref, twice_ref)
    lanes = iota((1, LANES), 1)
    row = jnp.where(lanes < 2, two_lanes(square, product, LANES), summed(gram_ref))
    send_ref[...] = jnp.broadcast_to(row, send_ref.shape)


def gram_kernel(devices, past_ref, send_ref):
    history = past_ref.shape[1]
    gram = jnp.zeros((history, history), F32)
    for c in range(past_ref.shape[0]):
        gram = gram + dot(past_ref[c], past_ref[c], ((1,), (1,)))
    chunk = history * history // devices
    send_ref[...] = jnp.zeros_like(send_ref)
    for d in range(devices):
        row, left = d * chunk // history, d * chunk % history
        send_ref[d : d + 1, 2 : 2 + chunk] = gram[row : row + 1, left : left + chunk]


def wall_next_kernel(devices, layers, rows, me_ref, near_ref, far_ref, state_ref, base_ref, stiff_ref,
                     send_ref, force_ref, image_ref, twice_ref, pull_ref):
    tiles, _, turns = base_ref.shape
    lead = (SUB - rows) // 2
    me = me_ref[0]
    even = (me & 1) == 0
    for c in range(3):
        near, far = near_ref[c : c + 1, :], far_ref[c : c + 1, :]
        low, high = jnp.where(even, far, near), jnp.where(even, near, far)
        for s in range(rows):
            pull_ref[c, lead + s : lead + s + 1, :] = state_ref[3 + c : 4 + c, s * turns : (s + 1) * turns]
        for s in range(lead):
            pull_ref[c, s : s + 1, :] = low[:, s * turns : (s + 1) * turns]
            pull_ref[c, lead + rows + s : lead + rows + s + 1, :] = high[:, s * turns : (s + 1) * turns]
    valid, own = row_masks(me, devices, rows, (SUB, turns))
    force = [base_ref[i] for i in range(tiles)]
    for c in range(3):
        force[c * layers] = force[c * layers] + pull_ref[c]
    stiff = [stiff_ref[i] for i in range(layers)]
    square, product = wall_parts(force, stiff, layers, valid, own, force_ref, image_ref, twice_ref)
    send_ref[...] = jnp.broadcast_to(two_lanes(square, product, LANES), (devices, LANES))


def summed(got_ref):
    return jnp.sum(got_ref[...], axis=0, keepdims=True)


def wall_second_kernel(rows, got_ref, force_ref, image_ref, twice_ref, send_ref):
    total = summed(got_ref)
    alpha = total[:, 0:1] / total[:, 1:2]
    shape = force_ref.shape[1:]
    lead = (SUB - rows) // 2
    sub = iota(shape, 0)
    own = (sub >= lead) & (sub < lead + rows)
    square = jnp.zeros(shape, F32)
    product = jnp.zeros(shape, F32)
    for i in range(force_ref.shape[0]):
        residual = force_ref[i] - alpha * image_ref[i]
        image = image_ref[i] - alpha * twice_ref[i]
        square = square + residual * residual
        product = product + residual * image
    square = jnp.sum(jnp.where(own, square, 0.0), keepdims=True)
    product = jnp.sum(jnp.where(own, product, 0.0), keepdims=True)
    lane = iota((1, LANES), 1)
    row = jnp.where(lane == 0, square, jnp.where(lane == 1, product, total))
    send_ref[...] = jnp.broadcast_to(row, send_ref.shape)


def wall_steps(at, one_ref, two_ref):
    one = summed(one_ref)
    two = jnp.sum(two_ref[:, at : at + 2], axis=0, keepdims=True)
    norm, alpha = one[:, 0:1], one[:, 0:1] / one[:, 1:2]
    newer = two[:, 0:1]
    ratio = newer / norm
    return alpha, newer / (two[:, 1:2] - ratio * newer / alpha), ratio


def moved_tile(index, steps, layers, rows, force_ref, image_ref, start_ref):
    alpha, beta, ratio = steps
    lead = (SUB - rows) // 2
    force = force_ref[index]
    residual = force - alpha * image_ref[index]
    moved = alpha * force + beta * (residual + ratio * force)
    return start_ref[index // layers, index % layers] + moved[lead : lead + rows, :]


def wall_last_kernel(layers, rows, at, one_ref, two_ref, force_ref, image_ref, start_ref, wall_ref):
    steps = wall_steps(at, one_ref, two_ref)
    for i in range(force_ref.shape[0]):
        wall_ref[i // layers, i % layers] = moved_tile(i, steps, layers, rows, force_ref, image_ref, start_ref)


def returned_kernel(devices, most, turn, layers, rows, got_ref, owner_ref, rank_ref, normals_ref, state_ref, past_ref,
                    one_ref, force_ref, image_ref, start_ref, *rest):
    if turn == 0:
        output_ref, resid_ref, send_ref = rest
    else:
        last_ref, output_ref, resid_ref, send_ref = rest
    named, placed = onehots(owner_ref[...], rank_ref[...], devices, most)
    spread = dot(got_ref[:, 0:most], named, ((0,), (0,)))
    sampled = jnp.sum(spread * placed, axis=0, keepdims=True)
    steps = wall_steps(most, one_ref, got_ref)
    turns = start_ref.shape[3]
    for c in range(3):
        tile = moved_tile(c * layers, steps, layers, rows, force_ref, image_ref, start_ref)
        for s in range(rows):
            output_ref[c : c + 1, s * turns : (s + 1) * turns] = tile[s : s + 1, :]
    output_ref[3:6, :] = -sampled * normals_ref[...]
    resid_ref[...] = output_ref[...] - state_ref[...]
    history = past_ref.shape[1]
    points = state_ref.shape[1]
    sub = iota((SUB, points), 0)
    parts = jnp.zeros((SUB, history), F32)
    newest = jnp.zeros((SUB, SUB), F32)
    for c in range(6):
        resid = resid_ref[c : c + 1, :]
        pair = jnp.where(sub == 0, resid, 0.0)
        if turn > 0:
            pair = jnp.where(sub == 1, resid - last_ref[c : c + 1, :], pair)
            newest = newest + dot(pair, pair, ((1,), (1,)))
        parts = parts + dot(pair, past_ref[c], ((1,), (1,)))
    send_ref[...] = jnp.zeros_like(send_ref)
    send_ref[:, 0:history] = jnp.broadcast_to(parts[0:1, :], (devices, history))
    if turn > 0:
        send_ref[:, history : 2 * history] = jnp.broadcast_to(parts[1:2, :], (devices, history))
        send_ref[:, 2 * history : 2 * history + 2] = jnp.broadcast_to(newest[1:2, 0:2], (devices, 2))


def gram_of(gram_ref, history, work_ref):
    devices = gram_ref.shape[0]
    chunk = history * history // devices
    for d in range(devices):
        row, left = d * chunk // history, d * chunk % history
        work_ref[row : row + 1, left : left + chunk] = gram_ref[d : d + 1, 2 : 2 + chunk]


def eliminated(table, history):
    sub, lane = iota(table.shape, 0), iota(table.shape, 1)
    diagonal = (sub == lane) & (sub < history)
    trace = jnp.sum(jnp.where(diagonal, table, 0.0), keepdims=True)
    ridge = RIDGE * trace / history + TINY
    table = jnp.where(diagonal, table + ridge, table)
    table = jnp.where((lane == sub + history) & (sub < history), 1.0, table)
    for k in range(0, history, 2):
        first, second = table[k : k + 1, :], table[k + 1 : k + 2, :]
        top, cross, low = first[:, k : k + 1], first[:, k + 1 : k + 2], second[:, k + 1 : k + 2]
        scale = 1.0 / (top * low - cross * cross)
        left = jnp.where(sub[:, 0:1] > k + 1, table[:, k : k + 1], 0.0)
        right = jnp.where(sub[:, 0:1] > k + 1, table[:, k + 1 : k + 2], 0.0)
        table = table - left * ((low * first - cross * second) * scale) - right * ((top * second - cross * first) * scale)
    return table[history:, history : 2 * history]


def inverse_kernel(history, gram_ref, out_ref, work_ref):
    work_ref[...] = jnp.zeros_like(work_ref)
    gram_of(gram_ref, history, work_ref)
    sub, lane = iota(work_ref.shape, 0), iota(work_ref.shape, 1)
    table = jnp.where((sub == lane + history) & (lane < history), 1.0, work_ref[...])
    out_ref[...] = eliminated(table, history)


def coefficients(history, got_ref, gram_ref, work_ref):
    total = summed(got_ref)
    work_ref[...] = jnp.zeros_like(work_ref)
    gram_of(gram_ref, history, work_ref)
    sub, lane = iota(work_ref.shape, 0), iota(work_ref.shape, 1)
    swap = history - 1
    fresh = total[:, history : 2 * history]
    square = total[:, 2 * history + 1 : 2 * history + 2]
    along = total[:, 2 * history : 2 * history + 1]
    edge = iota((1, history), 1) == swap
    work_ref[swap : swap + 1, 0:history] = jnp.where(edge, square, fresh)
    work_ref[history : history + 1, 0:history] = jnp.where(edge, along, total[:, 0:history])
    line = work_ref[swap : swap + 1, :]
    column = jnp.sum(jnp.where(sub == lane, line, 0.0), axis=1, keepdims=True)
    table = jnp.where((lane == swap) & (sub < history), column, work_ref[...])
    return eliminated(table, history)[0:1]


def update_kernel(devices, most, lead, turns, me_ref, got_ref, inverse_ref, output_ref, past_ref, owner_ref, rank_ref, normals_ref,
                  next_ref, send_ref, near_ref, far_ref):
    history = past_ref.shape[1]
    total = summed(got_ref)
    rows = dot(jnp.broadcast_to(total[:, 0:history], (SUB, history)), inverse_ref[...], ((1,), (0,)))
    for c in range(6):
        next_ref[c : c + 1, :] = output_ref[c : c + 1, :] + dot(rows, past_ref[c], ((1,), (0,)))[0:1, :]
    me = me_ref[0]
    points = output_ref.shape[1]
    named, placed = onehots(owner_ref[...], rank_ref[...], devices, most)
    flux = flux_of(normals_ref[...], next_ref[...])
    send_ref[...] = jnp.zeros_like(send_ref)
    send_ref[:, 0:most] = dot(named, placed * flux, ((1,), (1,)))
    half = lead * turns
    even = (me & 1) == 0
    for c in range(3):
        first, last = next_ref[3 + c : 4 + c, 0:half], next_ref[3 + c : 4 + c, points - half : points]
        near_ref[c : c + 1, :] = jnp.where(even, last, first)
        far_ref[c : c + 1, :] = jnp.where(even, first, last)


def finish_kernel(got_ref, gram_ref, output_ref, past_ref, last_ref, next_ref, work_ref):
    history = past_ref.shape[1]
    coeffs = coefficients(history, got_ref, gram_ref, work_ref)
    swap = history - 1
    newest = coeffs[:, swap:history]
    rows = jnp.broadcast_to(coeffs, (SUB, history))
    rows = jnp.where(iota(rows.shape, 1) == swap, 0.0, rows)
    for c in range(6):
        here = output_ref[c : c + 1, :]
        moved = dot(rows, past_ref[c], ((1,), (0,)))[0:1, :]
        next_ref[c : c + 1, :] = here + moved + newest * (here - last_ref[c : c + 1, :])


def local(
    pressure_start,
    fluid_coef,
    fluid_rhs,
    wall_start,
    wall_stiff,
    wall_load,
    normals,
    fluid_owner,
    fluid_cell,
    interface_start,
    past_residual,
    past_output,
):
    devices = lax.axis_size(AXES)
    me = lax.axis_index(AXES).astype(jnp.int32).reshape(1)
    rows, wide, depth = pressure_start.shape
    points = fluid_cell.shape[0]
    most = max(2, 2 * points // devices)
    history = past_residual.shape[0]
    layers, wall_rows, turns = wall_stiff.shape
    flat = (rows * wide, depth)
    plane = (wide, depth)
    lead = (SUB - wall_rows) // 2
    tiles = 3 * layers
    tile = (tiles, SUB, turns)
    slots = LANES * -(-2 * most // LANES)

    owner = fluid_owner.reshape(1, points)
    field = pressure_start.reshape(flat)
    low, high = field[0:wide], field[flat[0] - wide :]
    even = (me[0] & 1) == 0
    ends = tie(jnp.where(even, high, low), jnp.where(even, low, high))
    near, far = swap(*ends)
    past_r = jnp.transpose(past_residual, (1, 0, 2))
    past_w = jnp.transpose(past_output, (1, 0, 2))
    rhs = fluid_rhs.reshape(flat)

    owner, _ = tie(owner, ends)
    send, rank = call(
        functools.partial(route_kernel, devices, most),
        [((devices, slots), F32), ((1, points), jnp.int32)],
        [vmem()] * 4, limit=4,
    )(owner, fluid_cell.reshape(1, points), normals, interface_start)
    got = exchange(send)
    got, start_in, load_in, state = tie(got, wall_start, wall_load, interface_start)
    into, cells = places(jnp.maximum(got[:, 0:most].astype(jnp.int32) - 1, 0), flat[0], depth)
    thin = (flat[0] * depth // LANES, LANES)
    flux, spot = got, most
    scale = fluid_coef.reshape(flat)

    needed = (3 * (lead + 1) + 3 * lead + lead) * layers + 3 * lead
    packed = (SUB * -(-needed // SUB), turns)
    gram = call(functools.partial(gram_kernel, devices), [((devices, LANES), F32)], [vmem()], limit=4)(past_r)[0]
    packs = call(
        functools.partial(pack_kernel, layers, wall_rows),
        [(packed, F32)] * 2, [smem()] + [vmem()] * 4, [pltpu.VMEM((3, wall_rows, turns), F32)], limit=2,
    )(me, start_in, load_in, wall_stiff, state)

    small = ((devices, LANES), F32)
    padded = LANES * -(-2 * history // LANES)
    output = resid = None
    for turn in range(COUPLE):
        for sweep in range(SWEEPS):
            last = sweep + 1 == SWEEPS
            sending = not last or turn + 1 < COUPLE
            opening, closing = sweep == 0, not sending
            carrying, fetching = turn > 0, opening and turn == 0
            big = pl.BlockSpec(memory_space=pl.ANY) if fetching else vmem()
            extra_in, extra_spec, extra_out, scratch = [], [], [], []
            if opening:
                extra_in, extra_spec = [into, flux], [smem(), smem()]
                extra_out = [(flat, F32)] * (2 if turn == 0 else 1)
                scratch = [pltpu.VMEM(thin, F32)] * GRIDS
                if turn == 0:
                    scratch = scratch + [pltpu.VMEM(flat, F32)] * 3 + [pltpu.SemaphoreType.DMA((3,))]
            if closing:
                extra_in, extra_spec = [cells], [smem()]
                if carrying:
                    sums = call(
                        functools.partial(wall_second_kernel, wall_rows),
                        [((SUB, LANES), F32)], [vmem()] * 4, limit=2,
                    )(one, force, image, twice)[0]
                    extra_in, extra_spec = [cells, sums], [smem(), vmem()]
                extra_out = [((devices, LANES * -(-(most + 2) // LANES)), F32)]
                scratch = [pltpu.VMEM((devices * most, LANES), F32), pltpu.VMEM(thin, F32)]
            field, *rest = call(
                functools.partial(sweep_kernel, rows, most, spot, opening, closing, sending, carrying, fetching),
                [(flat if closing else thin, F32)] + [(plane, F32)] * (2 if sending else 0) + extra_out,
                [smem(), big, vmem(), vmem(), big, big] + extra_spec, scratch, limit=(44 if fetching else 26) if opening else 12,
            )(me, field, near, far, rhs if opening else source, scale, *extra_in)
            if sending:
                ends, rest = rest[:2], rest[2:]
            if opening:
                source = rest[0]
                scale = rest[-1] if fetching else scale
            if closing:
                sampled = rest[0]
            elif last:
                near, far = swap(*ends)
                sampled = call(
                    functools.partial(gather_kernel, most),
                    [((devices, LANES * -(-(most + 2) // LANES)), F32)],
                    [smem(), vmem(), vmem()],
                    [pltpu.VMEM((devices * most, LANES), F32)],
                    limit=12,
                )(cells, field, sums)[0]
            else:
                near, far = swap(*ends)
            if turn == 0 and sweep == 0:
                packs, _ = tie(packs, ends)
                pack_near, pack_far = swap(*packs)
                gram, _ = tie(gram, ends)
                gram = exchange(gram)
                far, pack_far, gram = tie(far, pack_far, gram)
            if turn == 0 and sweep == 1:
                pack_near, ends = tie(pack_near, ends)
                sums, base, stiff, force, image, twice = call(
                    functools.partial(wall_first_kernel, devices, layers),
                    [small, (tile, F32), ((layers, SUB, turns), F32)] + [(tile, F32)] * 3,
                    [smem()] + [vmem()] * 7,
                    [pltpu.VMEM((2 * tiles + layers + 3, SUB, turns), F32)], limit=6,
                )(me, start_in, load_in, wall_stiff, state, pack_near, pack_far, gram)
                one = exchange(sums)
                one, far = tie(one, far)
            if turn == 0 and sweep == 2:
                one, ends = tie(one, ends)
                sums = call(
                    functools.partial(wall_second_kernel, wall_rows),
                    [((SUB, LANES), F32)], [vmem()] * 4, limit=2,
                )(one, force, image, twice)[0]
                inverse = call(
                    functools.partial(inverse_kernel, history),
                    [((history, history), F32)], [vmem()], [pltpu.VMEM((2 * history, padded), F32)], limit=2,
                )(one)[0]
                inverse, far, sums = tie(inverse, far, sums)
                grams = one
            if turn == 1 and sweep == 0:
                pulls, ends = tie(pulls, ends)
                pull_near, pull_far = swap(*pulls)
                far, pull_far = tie(far, pull_far)
            if turn == 1 and sweep == 1:
                pull_near, ends = tie(pull_near, ends)
                sums, force, image, twice = call(
                    functools.partial(wall_next_kernel, devices, layers, wall_rows),
                    [small, (tile, F32), (tile, F32), (tile, F32)],
                    [smem()] + [vmem()] * 5,
                    [pltpu.VMEM((3, SUB, turns), F32)], limit=2,
                )(me, pull_near, pull_far, state, base, stiff)
                one = exchange(sums)
                one, far = tie(one, far)
        back = exchange(sampled)
        last_args = () if turn == 0 else (resid,)
        before = output
        output, resid, sums = call(
            functools.partial(returned_kernel, devices, most, turn, layers, wall_rows),
            [((6, points), F32), ((6, points), F32), ((devices, LANES * -(-(2 * history + 2) // LANES)), F32)],
            [vmem()] * (10 + len(last_args)), limit=4,
        )(back, owner, rank, normals, state, past_r, one, force, image, wall_start, *last_args)
        if turn + 1 < COUPLE:
            sums, inverse = tie(sums, inverse)
        total = exchange(sums)
        if turn + 1 < COUPLE:
            state, flux, *pulls = call(
                functools.partial(update_kernel, devices, most, lead, turns),
                [((6, points), F32), ((devices, LANES * -(-most // LANES)), F32)] + [((3, lead * turns), F32)] * 2,
                [smem()] + [vmem()] * 7, limit=4,
            )(me, total, inverse, output, past_w, owner, rank, normals)
            flux, spot = exchange(flux), 0
            flux, pulls = tie(flux, pulls)
        else:
            wall = call(
                functools.partial(wall_last_kernel, layers, wall_rows, most),
                [(wall_start.shape, F32)], [vmem()] * 5, limit=2,
            )(one, back, force, image, wall_start)[0]
            work = [pltpu.VMEM((SUB * -(-(history + 1) // SUB), padded), F32)]
            state = call(
                finish_kernel, [((6, points), F32)], [vmem()] * 5, work, limit=4,
            )(total, grams, output, past_w, before)[0]
    return (state, field.reshape(pressure_start.shape), wall)


def solution(mesh):
    placed = (
        P(("solver", "space"), None, None),
        P(("solver", "space"), None, None),
        P(("solver", "space"), None, None),
        P(None, None, ("solver", "space"), None),
        P(None, ("solver", "space"), None),
        P(None, None, ("solver", "space"), None),
        P(None, ("solver", "space")),
        P(("solver", "space"), None),
        P(("solver", "space")),
        P(None, ("solver", "space")),
        P(None, None, ("solver", "space")),
        P(None, None, ("solver", "space")),
    )

    return jax.shard_map(
        local,
        mesh=mesh,
        in_specs=placed,
        out_specs=(
            P(None, ("solver", "space")),
            P(("solver", "space"), None, None),
            P(None, None, ("solver", "space"), None),
        ),
        check_vma=False,
    )
```
